32 devices in a mesh: dp: 8 (over z, y), mp: 4 (over x, core).
Axes of the slice: x: 2, y: 2, z: 4, core: 2. Of those that a mesh axis runs over, the one named last changes fastest.
Arguments:
- clip_feats: bfloat16 [8192, 768], P('dp'), may hold values from -6 to 6
- counts: int32 [8], P('dp'), may hold values from 102 to 1024, as said below
- gain_one: bfloat16 [768], replicated, may hold values from 0.5 to 1.5
- shift_one: bfloat16 [768], replicated, may hold values from -1 to 1
- q_weight: bfloat16 [768, 768], P(None, 'mp'), may hold values from -0.21875 to 0.21875
- k_weight: bfloat16 [768, 768], P(None, 'mp'), may hold values from -0.21875 to 0.21875
- v_weight: bfloat16 [768, 768], P(None, 'mp'), may hold values from -0.21875 to 0.21875
- q_bias: bfloat16 [768], P('mp'), may hold values from -3 to 3
- v_bias: bfloat16 [768], P('mp'), may hold values from -0.59765625 to 0.59765625
- o_weight: bfloat16 [768, 768], P('mp'), may hold values from -1.75 to 1.75
- o_bias: bfloat16 [768], replicated, may hold values from -1.5 to 1.5
- gain_two: bfloat16 [768], replicated, may hold values from 0.5 to 1.5
- shift_two: bfloat16 [768], replicated, may hold values from -1 to 1
- up_weight: bfloat16 [768, 3072], P(None, 'mp'), may hold values from -0.21875 to 0.21875
- up_bias: bfloat16 [3072], P('mp'), may hold values from -3 to 3
- down_weight: bfloat16 [3072, 768], P('mp'), may hold values from -0.109375 to 0.109375
- down_bias: bfloat16 [768], replicated, may hold values from -1.5 to 1.5
- out_grad: bfloat16 [8192, 768], P('dp'), may hold values from -6 to 6
Outputs:
- layer_out: bfloat16 [8192, 768], P(('dp', 'mp'))
- feats_grad: bfloat16 [8192, 768], P(('dp', 'mp'))
- gain_one_grad: float32 [768], P(('dp', 'mp'))
- shift_one_grad: float32 [768], P(('dp', 'mp'))
- q_weight_grad: float32 [768, 768], P('dp', 'mp')
- k_weight_grad: float32 [768, 768], P('dp', 'mp')
- v_weight_grad: float32 [768, 768], P('dp', 'mp')
- q_bias_grad: float32 [768], P(('mp', 'dp'))
- v_bias_grad: float32 [768], P(('mp', 'dp'))
- o_weight_grad: float32 [768, 768], P('mp', 'dp')
- o_bias_grad: float32 [768], P(('dp', 'mp'))
- gain_two_grad: float32 [768], P(('dp', 'mp'))
- shift_two_grad: float32 [768], P(('dp', 'mp'))
- up_weight_grad: float32 [768, 3072], P('dp', 'mp')
- up_bias_grad: float32 [3072], P(('mp', 'dp'))
- down_weight_grad: float32 [3072, 768], P('mp', 'dp')
- down_bias_grad: float32 [768], P(('dp', 'mp'))
The draws below stay inside these ranges and needn't reach their ends.
Inputs may be any that keep to these rules, and one draw needn't show every extreme that they name: `counts`: the true patch count of each clip; some clip fills all 1024 slots.
All inputs are finite; a program needn't handle non-finite values.
Results may differ from the reference program's by a relative error of at most 0.02.
Values may be sent and summed in bfloat16 or wider, within the bound.
A program may use at most 128 MiB of HBM per device.

```python
import jax
import jax.numpy as jnp
from jax import lax

D = 768
H = 12
HD = 64
FF = 3072
SLOTS = 1024
CLIPS = 8
ROWS = 8192


def draw_counts(key, part):
    lengths = jax.random.randint(jax.random.fold_in(key, 11), (CLIPS,), max(1, SLOTS // 10), SLOTS + 1)
    filled = jax.random.randint(jax.random.fold_in(key, 12), (), 0, CLIPS)
    return jnp.where(jnp.arange(CLIPS, dtype=jnp.int32) == filled, SLOTS, lengths).astype(jnp.int32)


def levels(own_key, extent, shards, low, largest):
    factor_of = 1.0
    for dim, shards_of in shards:
        draws = jax.random.uniform(jax.random.fold_in(jax.random.fold_in(own_key, 6), dim), (shards_of,), jnp.float32, low / len(shards), largest / len(shards))
        factor_of = factor_of * jnp.repeat(jnp.exp(draws), extent[dim] // shards_of).reshape((-1,) + (1,) * (len(extent) - 1 - dim))
    return factor_of


def noise(stream_key, extent, deviation, limit, cuts=(), kind=jnp.bfloat16):
    values = jax.random.normal(stream_key, extent, jnp.float32) * deviation
    if len(cuts) > 0:
        values = levels(stream_key, extent, cuts, -0.22, 0.18) * values
    return jnp.clip(values, min=-limit, max=limit).astype(kind)


def setup_inputs(seed: int = 0) -> dict:
    keys = jax.random.split(jax.random.key(seed), 19)
    clip_feats = noise(keys[0], (ROWS, D), 1.0, 6.0, ((0, 8),))
    counts = draw_counts(jax.random.fold_in(keys[18], 71), 0)
    gain_one = jnp.clip(1.0 + 0.1 * jax.random.normal(keys[2], (D,), jnp.float32), 0.5, 1.5).astype(jnp.bfloat16)
    shift_one = noise(keys[3], (D,), 0.2, 1.0)
    q_weight = noise(keys[4], (D, D), D ** -0.5, 0.21875, ((1, 4),))
    k_weight = noise(keys[5], (D, D), D ** -0.5, 0.21875, ((1, 4),))
    v_weight = noise(keys[6], (D, D), D ** -0.5, 0.21875, ((1, 4),))
    q_bias = noise(keys[7], (D,), 0.5, 3.0, ((0, 4),))
    v_bias = noise(keys[8], (D,), 0.1, 0.59765625, ((0, 4),))
    o_weight = noise(keys[9], (D, D), (D // 64) ** -0.5, 1.75, ((0, 4),))
    o_bias = noise(keys[10], (D,), 0.3, 1.5)
    gain_two = jnp.clip(1.0 + 0.1 * jax.random.normal(keys[11], (D,), jnp.float32), 0.5, 1.5).astype(jnp.bfloat16)
    shift_two = noise(keys[12], (D,), 0.2, 1.0)
    up_weight = noise(keys[13], (D, FF), D ** -0.5, 0.21875, ((1, 4),))
    up_bias = noise(keys[14], (FF,), 0.5, 3.0, ((0, 4),))
    down_weight = noise(keys[15], (FF, D), FF ** -0.5, 0.109375, ((0, 4),))
    down_bias = noise(keys[16], (D,), 0.3, 1.5)
    out_grad = noise(keys[17], (ROWS, D), 1.0, 6.0, ((0, 8),))
    return {"clip_feats": clip_feats, "counts": counts, "gain_one": gain_one, "shift_one": shift_one, "q_weight": q_weight, "k_weight": k_weight, "v_weight": v_weight, "q_bias": q_bias, "v_bias": v_bias, "o_weight": o_weight, "o_bias": o_bias, "gain_two": gain_two, "shift_two": shift_two, "up_weight": up_weight, "up_bias": up_bias, "down_weight": down_weight, "down_bias": down_bias, "out_grad": out_grad}


NORM_EPSILON = 1e-06
SCORE_SCALE = 0.125
HIGHEST_PREC = lax.Precision.HIGHEST

@jax.custom_vjp
def low(v):
    return lax.optimization_barrier(v.astype(jnp.bfloat16)).astype(jnp.float32)

@jax.custom_vjp
def low_back(v):
    return v

def low_keep(v):
    return (low(v), None)

def low_pass(kept, grad):
    return (grad,)

def back_keep(v):
    return (v, None)

def back_low(kept, grad):
    return (low(grad),)
low.defvjp(low_keep, low_pass)
low_back.defvjp(back_keep, back_low)

def standardize(values):
    centered = values - lax.optimization_barrier(jnp.mean(values, axis=-1, keepdims=True))
    variance = lax.optimization_barrier(jnp.mean(centered * centered, axis=-1, keepdims=True))
    return centered * lax.rsqrt(variance + NORM_EPSILON)

def matmul(left, right):
    return jnp.dot(left, right, precision=HIGHEST_PREC)

def clip_layer(feats, clip_len, gain_one, shift_one, q_weight, k_weight, v_weight, q_bias, v_bias, o_weight, o_bias, gain_two, shift_two, up_weight, up_bias, down_weight, down_bias):
    normed = low(standardize(feats) * gain_one + shift_one)
    query = low(low_back(matmul(normed, q_weight) + q_bias)).reshape(SLOTS, H, HD)
    keys_all = low(low_back(matmul(normed, k_weight))).reshape(SLOTS, H, HD)
    values_all = low(low_back(matmul(normed, v_weight) + v_bias)).reshape(SLOTS, H, HD)
    scores = low_back(jnp.einsum('qhd,khd->hqk', query, keys_all, precision=HIGHEST_PREC) * SCORE_SCALE)
    key_live = jnp.arange(SLOTS, dtype=jnp.int32) < clip_len
    scores = jnp.where(key_live[None, None, :], scores, -1e+30)
    peak_score = lax.optimization_barrier(jnp.max(scores, axis=-1, keepdims=True))
    exp_scores = jnp.exp(scores - peak_score)
    probs = low(exp_scores / lax.optimization_barrier(jnp.sum(exp_scores, axis=-1, keepdims=True)))
    mixed = jnp.einsum('hqk,khd->qhd', probs, values_all, precision=HIGHEST_PREC).reshape(SLOTS, D)
    mixed = low(low_back(mixed))
    resid = feats + low_back(matmul(mixed, o_weight) + o_bias)
    normed_two = low(standardize(resid) * gain_two + shift_two)
    pre_up = low_back(matmul(normed_two, up_weight) + up_bias)
    hidden = low(jax.nn.gelu(pre_up, approximate=False))
    return resid + low_back(matmul(hidden, down_weight) + down_bias)

def reference(clip_feats, counts, gain_one, shift_one, q_weight, k_weight, v_weight, q_bias, v_bias, o_weight, o_bias, gain_two, shift_two, up_weight, up_bias, down_weight, down_bias, out_grad):
    params = tuple((weight.astype(jnp.float32) for weight in (gain_one, shift_one, q_weight, k_weight, v_weight, q_bias, v_bias, o_weight, o_bias, gain_two, shift_two, up_weight, up_bias, down_weight, down_bias)))
    feats_all = clip_feats.astype(jnp.float32).reshape(CLIPS, SLOTS, D)
    grads_all = out_grad.astype(jnp.float32).reshape(CLIPS, SLOTS, D)

    def one_clip(totals, pieces):
        feats, clip_len, grad_rows = pieces
        row_live = (jnp.arange(SLOTS, dtype=jnp.int32) < clip_len)[:, None]
        grad_rows = jnp.where(row_live, grad_rows, jnp.zeros_like(grad_rows))
        layer_value, pull_back = jax.vjp(lambda clip_in, *weights: clip_layer(clip_in, clip_len, *weights), feats, *params)
        pulled = pull_back(grad_rows)
        totals = tuple((total + part for total, part in zip(totals, pulled[1:])))
        return (totals, (layer_value.astype(jnp.bfloat16), pulled[0].astype(jnp.bfloat16)))
    start_totals = tuple((jnp.zeros_like(weight) for weight in params))
    totals, (outs_all, feat_grads) = lax.scan(one_clip, start_totals, (feats_all, counts, grads_all))
    return (outs_all.reshape(CLIPS * SLOTS, D), feat_grads.reshape(CLIPS * SLOTS, D), totals[0], totals[1], totals[2], totals[3], totals[4], totals[5], totals[6], totals[7], totals[8], totals[9], totals[10], totals[11], totals[12], totals[13], totals[14])
```

```python
import functools
import types

import jax
import jax.numpy as jnp
from jax import lax
from jax.experimental import pallas as pl
from jax.experimental.pallas import tpu as pltpu
from jax.sharding import PartitionSpec as P

HD = 64
NORM_EPSILON = 1e-06
SCORE_SCALE = 0.125
BLOCK = 256
MESH = pl.DeviceIdType.MESH
F32 = jnp.float32
BF16 = jnp.bfloat16
INV_SQRT2 = 0.7071067811865476
INV_SQRT_2PI = 0.3989422804014327
NEG = -1e30

PIECES = (("down", (0, 1, 2)), ("up", (1, 0, 2)), ("qk", (0, 1, 2)), ("vo", (1, 0, 2)))


def dot(left, right):
    return jnp.dot(left, right, preferred_element_type=F32)


def dot_nt(left, right):
    return lax.dot_general(left, right, (((1,), (1,)), ((), ())), preferred_element_type=F32)


def dot_tn(left, right):
    return lax.dot_general(left, right, (((0,), (0,)), ((), ())), preferred_element_type=F32)


def standardized(values):
    centered = values - jnp.mean(values, axis=-1, keepdims=True)
    variance = jnp.mean(centered * centered, axis=-1, keepdims=True)
    inverse = lax.rsqrt(variance + NORM_EPSILON)
    return centered * inverse, inverse


def norm_back(std_rows, inverse, gain, grad):
    scaled = gain * grad
    mean_scaled = jnp.mean(scaled, axis=-1, keepdims=True)
    mean_inner = jnp.mean(scaled * std_rows, axis=-1, keepdims=True)
    return inverse * (scaled - mean_scaled - std_rows * mean_inner)


def gelu_pair(values):
    bell = jnp.exp(-0.5 * (values * values))
    t = 1.0 / (1.0 + (0.3275911 * INV_SQRT2) * jnp.abs(values))
    tail = t * (0.127414796 + t * (-0.142248368 + t * (0.7107068705 + t * (-0.7265760135 + t * 0.5307027145)))) * bell
    phi = jnp.where(values >= 0.0, 1.0 - tail, tail)
    return values * phi, phi + values * (bell * INV_SQRT_2PI)


def column_sum(values):
    return jnp.sum(values, axis=0, keepdims=True)


def row_of(ref):
    return ref[...].astype(F32).reshape(1, -1)


def layer_kernel(names, dp_bits, *refs):
    r = types.SimpleNamespace(**dict(zip(names, refs)))
    rows, width = r.feats_hbm.shape
    cols = r.qw_hbm.shape[1]
    hidden_cols = r.up_hbm.shape[1]
    heads = cols // HD
    blocks = rows // BLOCK

    m = lax.axis_index("mp")
    c = m % 2
    x = m // 2
    cp = m + 1 - 2 * c
    xp = m + 2 - 4 * x
    count = r.counts[0]

    def bit_of(bit):
        return (lax.axis_index("dp") // (1 << bit)) % 2

    def dp_partner(bit):
        return lax.axis_index("dp") + (1 << bit) * (1 - 2 * bit_of(bit))

    loads = [
        ("feats_hbm", r.feats), ("qw_hbm", r.qw), ("kw_hbm", r.kw), ("vw_hbm", r.vw),
        ("ow_hbm", r.ow.at[pl.ds(pl.multiple_of(m * cols, 64), cols), :]), ("og_hbm", r.og),
        ("down_hbm", r.down), ("up_hbm", r.up),
    ]

    def load(i):
        return pltpu.make_async_copy(getattr(r, loads[i][0]), loads[i][1], r.load_sem.at[i])

    for i in range(len(loads)):
        load(i).start()

    barrier = pltpu.get_barrier_semaphore()
    partners = [{"mp": cp}, {"mp": xp}] + [{"dp": dp_partner(bit)} for bit in range(dp_bits)]
    for partner in partners:
        pl.semaphore_signal(barrier, inc=1, device_id=partner, device_id_type=MESH)
    pl.semaphore_wait(barrier, len(partners))

    def remote(index, source, target, partner):
        return pltpu.make_async_remote_copy(
            src_ref=source, dst_ref=target, send_sem=r.send_sem.at[index], recv_sem=r.recv_sem.at[index],
            device_id=partner, device_id_type=MESH,
        )

    def rows_at(start, size):
        return pl.ds(pl.multiple_of(start, size), size)

    OW, MX, RL, BK, ML, IN, SM = 0, 3, 12, 15, 18, 21, 24
    DP = SM + dp_bits + 2

    def ow_copy(kind):
        owner = (m, m, xp)[kind]
        view = r.ow.at[rows_at(owner * cols, 64 * 3), :]
        return remote(OW + kind, view, view, {"mp": (cp, xp, cp)[kind]})

    def mx_copy(kind, h):
        owner = (m, m, xp)[kind]
        view = r.mixed_t.at[rows_at(owner * cols + h * HD, HD), :]
        return remote(MX + kind * 3 + h, view, view, {"mp": (cp, xp, cp)[kind]})

    def rl_copy(kind):
        owner = (m, m, xp)[kind]
        view = r.resid_low.at[rows_at(owner * BLOCK, BLOCK), :]
        return remote(RL + kind, view, view, {"mp": (cp, xp, cp)[kind]})

    def rs_copy(base, step):
        send, receive = {BK: (r.bk_tx, r.bk_rx), ML: (r.ml_tx, r.ml_rx), IN: (r.in_tx, r.in_rx)}[base]
        return remote(base + step, send.at[step], receive.at[step], {"mp": (cp, xp, cp)[step]})

    def block_of(k):
        kx, kc = k // 2, k % 2
        return 2 * (x + kx - 2 * x * kx) + (c + kc - 2 * c * kc)

    piece_index = {name: i for i, (name, _) in enumerate(PIECES)}

    def store_piece(name, tile, value, column):
        if not dp_bits:
            target = getattr(r, "g_" + name)
            target[pl.ds(tile * 384, 384), column : column + value.shape[1]] = value
            return
        order = PIECES[piece_index[name]][1]
        weight = {bit: 1 << (len(order) - 1 - place) for place, bit in enumerate(order)}
        target = getattr(r, "b0_" + name)
        for j in range(4):
            place = (j % 2) * weight[0] + (j // 2) * weight[1] + tile * weight[2]
            target[place, :, column : column + value.shape[1]] = value[j * 96 : (j + 1) * 96].astype(BF16)

    def dp_copy(name, stage):
        order = PIECES[piece_index[name]][1]
        bit = order[stage]
        count_here = 4 >> stage
        source = getattr(r, f"b{stage}_{name}").at[pl.ds((1 - bit_of(bit)) * count_here, count_here)]
        target = getattr(r, f"x{stage}_{name}")
        return remote(DP + 3 * piece_index[name] + stage, source, target, {"dp": dp_partner(bit)})

    def dp_start(name, stage):
        if dp_bits:
            dp_copy(name, stage).start()

    def dp_finish(name, stage):
        if not dp_bits:
            return
        order = PIECES[piece_index[name]][1]
        count_here = 4 >> stage
        mine = bit_of(order[stage]) * count_here
        dp_copy(name, stage).wait_recv()
        kept = getattr(r, f"b{stage}_{name}")
        arrived = getattr(r, f"x{stage}_{name}")
        for i in range(count_here):
            total = kept[mine + i].astype(F32) + arrived[i].astype(F32)
            if stage < 2:
                getattr(r, f"b{stage + 1}_{name}")[i] = total.astype(BF16)
            else:
                getattr(r, "g_" + name)[...] = total
        if stage < 2:
            dp_copy(name, stage + 1).start()

    load(4).wait()
    ow_copy(0).start()
    ow_copy(1).start()

    for i in (0, 1, 2, 3):
        load(i).wait()
    r.wqkv[...] = jnp.concatenate([r.qw[...], r.kw[...], r.vw[...]], axis=1)
    gain_one, shift_one = row_of(r.gain_one), row_of(r.shift_one)
    q_bias, v_bias = row_of(r.q_bias), row_of(r.v_bias)
    lane = lax.broadcasted_iota(jnp.int32, (BLOCK, HD), 1)
    row_in_block = lax.broadcasted_iota(jnp.int32, (BLOCK, HD), 0)

    @pl.loop(0, blocks)
    def _(i):
        here = rows_at(i * BLOCK, BLOCK)
        std_rows, _ = standardized(r.feats[here, :].astype(F32))
        normed = (std_rows * gain_one + shift_one).astype(BF16)
        r.normed[here, :] = normed
        projected = dot(normed, r.wqkv[...])
        query = ((projected[:, :cols] + q_bias).astype(BF16).astype(F32) * SCORE_SCALE).astype(BF16)
        keys = projected[:, cols : 2 * cols].astype(BF16)
        values = (projected[:, 2 * cols :] + v_bias).astype(BF16)
        one = jnp.where(lane == 0, 1.0, 0.0).astype(BF16)
        bias = jnp.where(jnp.logical_and(lane == 0, row_in_block + i * BLOCK >= count), NEG, 0.0).astype(BF16)
        for h in range(heads):
            part = slice(h * HD, (h + 1) * HD)
            r.query[h, here, :] = jnp.concatenate([query[:, part], one], axis=1)
            r.keys[h, here, :] = jnp.concatenate([keys[:, part], bias], axis=1)
            r.values[h, here, :] = values[:, part]
        keys_t = keys.T
        values_t = values.T
        for h in range(heads):
            part = slice(h * HD, (h + 1) * HD)
            r.keys_t[h, :, here] = keys_t[part, :]
            r.values_t[h, :, here] = values_t[part, :]

    def mx_forward(h):
        mx_copy(1, h).wait_recv()
        mx_copy(2, h).start()

    @pl.loop(0, heads)
    def _(h):
        @pl.loop(0, blocks)
        def _(j):
            here = rows_at(j * BLOCK, BLOCK)
            scores = dot_nt(r.keys[h], r.query[h, here, :])
            peak = jnp.max(scores, axis=0, keepdims=True)
            exped = jnp.exp(scores - peak)
            total = jnp.sum(exped, axis=0, keepdims=True)
            mixed = dot(r.values_t[h], exped.astype(BF16)) / total
            r.mixed_t[pl.ds(pl.multiple_of(m * cols + h * HD, HD), HD), here] = mixed.astype(BF16)
            r.lse[h, :, here] = peak + jnp.log(total)

        mx_copy(0, h).start()
        mx_copy(1, h).start()

        @pl.when(h > 0)
        def _():
            mx_forward(h - 1)

    ow_copy(1).wait_recv()
    ow_copy(2).start()
    for i in (5, 6, 7):
        load(i).wait()
    slot = lax.broadcasted_iota(jnp.int32, (BLOCK, width), 0)

    @pl.loop(0, blocks)
    def _(i):
        here = rows_at(i * BLOCK, BLOCK)
        grad = r.og[here, :]
        grad = jnp.where(slot + i * BLOCK < count, grad.astype(F32), 0.0).astype(BF16)
        r.og[here, :] = grad
        r.hidden_grad[here, :] = dot_nt(grad, r.down[...])

    mx_forward(heads - 1)
    for h in range(heads):
        mx_copy(0, h).wait_recv()
        mx_copy(2, h).wait_recv()
    ow_copy(0).wait_recv()
    ow_copy(2).wait_recv()

    o_bias = row_of(r.o_bias)
    gain_two, shift_two = row_of(r.gain_two), row_of(r.shift_two)
    up_bias, down_bias = row_of(r.up_bias), row_of(r.down_bias)
    r.up_bias_sum[...] = jnp.zeros_like(r.up_bias_sum)

    @pl.loop(0, blocks)
    def _(i):
        here = rows_at(block_of(3 - i) * BLOCK, BLOCK)
        attended = dot_tn(r.mixed_t[:, here], r.ow[...])
        resid = r.feats[here, :].astype(F32) + (attended + o_bias)
        std_rows, _ = standardized(resid)
        normed_two = (std_rows * gain_two + shift_two).astype(BF16)
        r.normed_two[here, :] = normed_two
        pre_up = dot(normed_two, r.up[...]) + up_bias
        hidden, slope = gelu_pair(pre_up)
        r.hidden[here, :] = hidden.astype(BF16)
        pre_grad = (r.hidden_grad[here, :] * slope).astype(BF16)
        r.pre_grad[here, :] = pre_grad
        r.up_bias_sum[...] += column_sum(pre_grad.astype(F32))
        back = dot_nt(pre_grad, r.up[...])

        @pl.when(i == 0)
        def _():
            r.bk_tx[0] = back.astype(BF16)
            rs_copy(BK, 0).start()

        @pl.when(i == 1)
        def _():
            rs_copy(BK, 0).wait_recv()
            r.bk_tx[1] = (back + r.bk_rx[0].astype(F32)).astype(BF16)
            rs_copy(BK, 1).start()

        @pl.when(i == 2)
        def _():
            r.bk_tx[2] = back.astype(BF16)
            rs_copy(BK, 2).start()

        @pl.when(i == 3)
        def _():
            r.resid[...] = resid
            r.back[...] = back

    def grad_tiles(left, right, name, column):
        right_all = right[...]

        @pl.loop(0, 2)
        def _(t):
            value = dot_tn(left[:, rows_at(t * 384, 384)], right_all)
            store_piece(name, t, value, column)

    grad_tiles(r.og, r.hidden, "down", 0)
    dp_start("down", 0)

    own = rows_at(m * BLOCK, BLOCK)
    rs_copy(BK, 2).wait_recv()
    rs_copy(BK, 1).wait_recv()
    back = r.back[...] + r.bk_rx[2].astype(F32) + r.bk_rx[1].astype(F32)
    std_rows, inverse = standardized(r.resid[...])
    own_grad = r.og[own, :].astype(F32)
    resid_grad = own_grad + norm_back(std_rows, inverse, gain_two, back)
    resid_low = resid_grad.astype(BF16)
    r.resid_grad[...] = resid_grad
    r.resid_low[own, :] = resid_low
    rl_copy(0).start()
    rl_copy(1).start()
    r.small[2:3, :] = column_sum(resid_low.astype(F32))
    r.small[3:4, :] = column_sum(back * std_rows)
    r.small[4:5, :] = column_sum(back)
    r.small[5:6, :] = column_sum(own_grad)
    r.small[6:7, :] = r.up_bias_sum[...]

    grad_tiles(r.normed_two, r.pre_grad, "up", 0)
    dp_start("up", 0)

    @pl.loop(0, blocks)
    def _(i):
        here = rows_at(block_of(3 - i) * BLOCK, BLOCK)
        part = dot(r.hidden[here, :], r.down[...])

        @pl.when(i < 3)
        def _():
            r.ml_tx[i] = part.astype(BF16)

        @pl.when(i == 3)
        def _():
            r.ml_own[...] = part

        @pl.when(i == 0)
        def _():
            rs_copy(ML, 0).start()

        @pl.when(i == 2)
        def _():
            rs_copy(ML, 2).start()

    r.key_acc[...] = jnp.zeros_like(r.key_acc)
    r.value_acc[...] = jnp.zeros_like(r.value_acc)

    @pl.loop(0, blocks)
    def _(i):
        @pl.when(i == 1)
        def _():
            rl_copy(0).wait_recv()

        @pl.when(i == 2)
        def _():
            rl_copy(1).wait_recv()
            rl_copy(2).start()

        @pl.when(i == 3)
        def _():
            rl_copy(2).wait_recv()
            rs_copy(ML, 0).wait_recv()
            r.ml_tx[1] = (r.ml_tx[1].astype(F32) + r.ml_rx[0].astype(F32)).astype(BF16)
            rs_copy(ML, 1).start()
            dp_finish("down", 0)

        here = rows_at(block_of(i) * BLOCK, BLOCK)
        low = r.resid_low[here, :]
        ow_own = r.ow[rows_at(m * cols, 64 * 3), :]
        mixed_grad = dot_nt(low, ow_own).astype(BF16)
        mixed_grad_t = dot_nt(ow_own, low).astype(BF16).astype(F32)
        inner = mixed_grad_t * r.mixed_t[rows_at(m * cols, 64 * 3), here].astype(F32)
        for h in range(heads):
            r.mixed_grad[h] = mixed_grad[:, h * HD : (h + 1) * HD]
            r.inner[h] = column_sum(inner[h * HD : (h + 1) * HD])

        @pl.loop(0, heads)
        def _(h):
            query = r.query[h, here, :]
            grad = r.mixed_grad[h]
            scores = dot_nt(r.keys[h], query)
            probs = jnp.exp(scores - r.lse[h, :, here])
            prob_grad = dot_nt(r.values[h], grad)
            score_grad = (probs * (prob_grad - r.inner[h])).astype(BF16)
            r.value_acc[h] += dot(probs.astype(BF16), grad)
            r.key_acc[h] += dot(score_grad, query)
            query_grad = dot(r.keys_t[h], score_grad) * SCORE_SCALE
            r.query_grad[h, here, :] = query_grad.T.astype(BF16)

    dp_finish("up", 0)

    @pl.loop(0, blocks)
    def _(i):
        here = rows_at(i * BLOCK, BLOCK)
        parts = [r.query_grad[h, here, :] for h in range(heads)]
        parts += [r.key_acc[h, here, :][:, :HD].astype(BF16) for h in range(heads)]
        parts += [r.value_acc[h, here, :].astype(BF16) for h in range(heads)]
        r.dqkv[here, :] = jnp.concatenate(parts, axis=1)

    @pl.loop(0, 2)
    def _(t):
        columns = rows_at(t * 384, 384)
        value = dot_tn(r.normed[:, columns], r.dqkv[...])
        store_piece("qk", t, value[:, : 2 * cols], 0)
        store_piece("vo", t, value[:, 2 * cols :], 0)
        out_grad_t = dot(r.mixed_t[rows_at(m * cols, 64 * 3), :], r.resid_low[:, columns])
        store_piece("vo", t, out_grad_t.T, cols)

    dp_start("qk", 0)
    dp_start("vo", 0)
    dp_finish("down", 1)

    r.gain_sum[...] = jnp.zeros_like(r.gain_sum)
    r.shift_sum[...] = jnp.zeros_like(r.shift_sum)
    r.bias_sum[...] = jnp.zeros_like(r.bias_sum)

    @pl.loop(0, blocks)
    def _(i):
        here = rows_at(block_of(3 - i) * BLOCK, BLOCK)
        part_grads = r.dqkv[here, :]
        part = dot_nt(part_grads, r.wqkv[...])

        @pl.when(i == 0)
        def _():
            r.in_tx[0] = part.astype(BF16)
            rs_copy(IN, 0).start()

        @pl.when(i == 1)
        def _():
            rs_copy(IN, 0).wait_recv()
            r.in_tx[1] = (part + r.in_rx[0].astype(F32)).astype(BF16)
            rs_copy(IN, 1).start()

        @pl.when(i == 2)
        def _():
            r.in_tx[2] = part.astype(BF16)
            rs_copy(IN, 2).start()

        @pl.when(i == 3)
        def _():
            r.back[...] = part

        std_rows, _ = standardized(r.feats[here, :].astype(F32))
        r.gain_sum[...] += column_sum(part * std_rows)
        r.shift_sum[...] += column_sum(part)
        r.bias_sum[...] += column_sum(part_grads.astype(F32))

    r.small[0:1, :] = r.gain_sum[...]
    r.small[1:2, :] = r.shift_sum[...]
    r.small[7:8, :] = jnp.concatenate([r.bias_sum[...], jnp.zeros((1, width - 3 * cols), F32)], axis=1)

    sm_partners = [{"dp": dp_partner(bit)} for bit in range(dp_bits)] + [{"mp": cp}, {"mp": xp}]

    def sm_copy(stage):
        source = r.small if stage == 0 else r.sm_sum.at[stage - 1]
        return remote(SM + stage, source, r.sm_rx.at[stage], sm_partners[stage])

    def sm_finish(stage):
        sm_copy(stage).wait_recv()
        kept = r.small[...] if stage == 0 else r.sm_sum[stage - 1]
        arrived = r.sm_rx[stage]
        if stage >= dp_bits:
            arrived = jnp.where(lax.broadcasted_iota(jnp.int32, arrived.shape, 0) < 6, arrived, 0.0)
        total = kept + arrived
        if stage < len(sm_partners) - 1:
            r.sm_sum[stage] = total
            sm_copy(stage + 1).start()
        else:
            r.small_out[...] = total

    sm_copy(0).start()
    dp_finish("up", 1)
    rs_copy(ML, 1).wait_recv()
    rs_copy(ML, 2).wait_recv()
    mlp = r.ml_own[...] + r.ml_rx[2].astype(F32) + r.ml_rx[1].astype(F32)
    r.layer_out[...] = (r.resid[...] + (mlp + down_bias)).astype(BF16)
    sm_finish(0)
    dp_finish("qk", 0)
    dp_finish("vo", 0)
    sm_finish(1)
    rs_copy(IN, 2).wait_recv()
    rs_copy(IN, 1).wait_recv()
    back = r.back[...] + r.in_rx[2].astype(F32) + r.in_rx[1].astype(F32)
    std_rows, inverse = standardized(r.feats[own, :].astype(F32))
    r.feats_grad[...] = (r.resid_grad[...] + norm_back(std_rows, inverse, gain_one, back)).astype(BF16)
    for stage in range(2, len(sm_partners)):
        sm_finish(stage)
    dp_finish("qk", 1)
    dp_finish("vo", 1)
    for name, _ in PIECES:
        dp_finish(name, 2)

    for kind in range(3):
        ow_copy(kind).wait_send()
        rl_copy(kind).wait_send()
        for h in range(heads):
            mx_copy(kind, h).wait_send()
        for base in (BK, ML, IN):
            rs_copy(base, kind).wait_send()
    for stage in range(len(sm_partners)):
        sm_copy(stage).wait_send()
    if dp_bits:
        for name, _ in PIECES:
            for stage in range(3):
                dp_copy(name, stage).wait_send()


PIECE_COLUMNS = {"down": 768, "up": 768, "qk": 384, "vo": 384}


def layer_call(dp_size, clip_feats, counts, gain_one, shift_one, q_weight, k_weight, v_weight, q_bias, v_bias, o_weight,
               o_bias, gain_two, shift_two, up_weight, up_bias, down_weight, down_bias, out_grad):
    rows, width = clip_feats.shape
    cols = q_weight.shape[1]
    heads = cols // HD
    hidden_cols = up_weight.shape[1]
    dp_bits = 3 if dp_size == 8 else 0
    vmem = pl.BlockSpec(memory_space=pltpu.VMEM)
    anywhere = pl.BlockSpec(memory_space=pl.ANY)
    inputs = {
        "counts": (counts, pl.BlockSpec(memory_space=pltpu.SMEM)),
        "gain_one": (gain_one, vmem), "shift_one": (shift_one, vmem), "q_bias": (q_bias, vmem), "v_bias": (v_bias, vmem),
        "o_bias": (o_bias, vmem), "gain_two": (gain_two, vmem), "shift_two": (shift_two, vmem), "up_bias": (up_bias, vmem),
        "down_bias": (down_bias, vmem),
        "feats_hbm": (clip_feats, anywhere), "qw_hbm": (q_weight, anywhere), "kw_hbm": (k_weight, anywhere),
        "vw_hbm": (v_weight, anywhere), "ow_hbm": (o_weight, anywhere), "up_hbm": (up_weight, anywhere),
        "down_hbm": (down_weight, anywhere), "og_hbm": (out_grad, anywhere),
    }
    shard = width // dp_size if dp_bits else width
    outputs = {"layer_out": ((BLOCK, width), BF16), "feats_grad": ((BLOCK, width), BF16), "small_out": ((8, width), F32)}
    for name, _ in PIECES:
        outputs["g_" + name] = ((shard, PIECE_COLUMNS[name]), F32)
    piece = (BLOCK, width)
    scratch = {
        "feats": ((rows, width), BF16), "qw": ((width, cols), BF16), "kw": ((width, cols), BF16), "vw": ((width, cols), BF16),
        "wqkv": ((width, 3 * cols), BF16), "ow": ((width, width), BF16), "og": ((rows, width), BF16),
        "down": ((hidden_cols, width), BF16), "up": ((width, hidden_cols), BF16), "normed": ((rows, width), BF16),
        "query": ((heads, rows, 2 * HD), BF16), "keys": ((heads, rows, 2 * HD), BF16), "values": ((heads, rows, HD), BF16),
        "keys_t": ((heads, HD, rows), BF16), "values_t": ((heads, HD, rows), BF16), "mixed_t": ((width, rows), BF16),
        "lse": ((heads, 1, rows), F32), "hidden_grad": ((rows, hidden_cols), F32), "resid": (piece, F32),
        "normed_two": ((rows, width), BF16), "hidden": ((rows, hidden_cols), BF16), "pre_grad": ((rows, hidden_cols), BF16),
        "up_bias_sum": ((1, hidden_cols), F32), "back": (piece, F32), "resid_grad": (piece, F32),
        "resid_low": ((rows, width), BF16), "ml_own": (piece, F32),
        "bk_tx": ((3,) + piece, BF16), "bk_rx": ((3,) + piece, BF16), "ml_tx": ((3,) + piece, BF16),
        "ml_rx": ((3,) + piece, BF16), "in_tx": ((3,) + piece, BF16), "in_rx": ((3,) + piece, BF16),
        "mixed_grad": ((heads, BLOCK, HD), BF16), "inner": ((heads, 1, BLOCK), F32),
        "key_acc": ((heads, rows, 2 * HD), F32), "value_acc": ((heads, rows, HD), F32),
        "query_grad": ((heads, rows, HD), BF16), "dqkv": ((rows, 3 * cols), BF16),
        "gain_sum": ((1, width), F32), "shift_sum": ((1, width), F32), "bias_sum": ((1, 3 * cols), F32),
        "small": ((8, width), F32), "sm_sum": ((dp_bits + 1, 8, width), F32), "sm_rx": ((dp_bits + 2, 8, width), F32),
    }
    if dp_bits:
        for name, _ in PIECES:
            for stage in range(3):
                scratch[f"b{stage}_{name}"] = ((8 >> stage, shard, PIECE_COLUMNS[name]), BF16)
                scratch[f"x{stage}_{name}"] = ((4 >> stage, shard, PIECE_COLUMNS[name]), BF16)
    copies = 24 + dp_bits + 2 + 12
    names = list(inputs) + list(outputs) + list(scratch) + ["load_sem", "send_sem", "recv_sem"]
    results = pl.pallas_call(
        functools.partial(layer_kernel, names, dp_bits),
        out_shape=[jax.ShapeDtypeStruct(*spec) for spec in outputs.values()],
        in_specs=[spec for _, spec in inputs.values()],
        out_specs=[vmem] * len(outputs),
        scratch_shapes=[pltpu.VMEM(*spec) for spec in scratch.values()]
        + [pltpu.SemaphoreType.DMA((8,)), pltpu.SemaphoreType.DMA((copies,)), pltpu.SemaphoreType.DMA((copies,))],
        compiler_params=pltpu.CompilerParams(collective_id=0, has_side_effects=True, vmem_limit_bytes=67043328),
        name="layer",
    )(*[value for value, _ in inputs.values()])
    return dict(zip(outputs, results))


def shards(dp_size, *args):
    out = layer_call(dp_size, *args)
    cols = args[4].shape[1]
    small = out["small_out"]
    width = small.shape[1]
    d, m = lax.axis_index("dp"), lax.axis_index("mp")

    def over(value, dim):
        return value if dp_size == 8 else lax.psum_scatter(value, "dp", scatter_dimension=dim, tiled=True)

    if dp_size != 8:
        small = lax.psum(small, "dp")
    g_qk, g_vo = out["g_qk"], out["g_vo"]
    piece = width // (dp_size * 4)
    group = [lax.dynamic_slice(small, (i, (d * 4 + m) * piece), (1, piece)).reshape(piece) for i in range(6)]
    up_piece = args[14].shape[0] // dp_size
    head_piece = cols // dp_size
    up_bias = lax.dynamic_slice(small, (6, d * up_piece), (1, up_piece)).reshape(up_piece)
    q_bias = lax.dynamic_slice(small, (7, d * head_piece), (1, head_piece)).reshape(head_piece)
    v_bias = lax.dynamic_slice(small, (7, 2 * cols + d * head_piece), (1, head_piece)).reshape(head_piece)
    return (
        out["layer_out"], out["feats_grad"], group[0], group[1],
        over(g_qk[:, :cols], 0), over(g_qk[:, cols:], 0), over(g_vo[:, :cols], 0), q_bias, v_bias,
        over(g_vo[:, cols:].T, 1), group[2], group[3], group[4], over(out["g_up"], 0), up_bias, over(out["g_down"].T, 1),
        group[5],
    )


def solution(mesh):
    placed = (
        P("dp", None), P("dp"), P(), P(), P(None, "mp"), P(None, "mp"), P(None, "mp"), P("mp"), P("mp"), P("mp", None),
        P(), P(), P(), P(None, "mp"), P("mp"), P("mp", None), P(), P("dp", None),
    )
    return jax.shard_map(
        functools.partial(shards, mesh.shape["dp"]),
        mesh=mesh,
        in_specs=placed,
        out_specs=(
            P(("dp", "mp"), None), P(("dp", "mp"), None), P(("dp", "mp")), P(("dp", "mp")), P("dp", "mp"), P("dp", "mp"),
            P("dp", "mp"), P(("mp", "dp")), P(("mp", "dp")), P("mp", "dp"), P(("dp", "mp")), P(("dp", "mp")),
            P(("dp", "mp")), P("dp", "mp"), P(("mp", "dp")), P("mp", "dp"), P(("dp", "mp")),
        ),
        check_vma=False,
    )
```

```python
import functools
import types

import jax
import jax.numpy as jnp
from jax import lax
from jax.experimental import pallas as pl
from jax.experimental.pallas import tpu as pltpu
from jax.sharding import PartitionSpec as P

HD = 64
NORM_EPSILON = 1e-06
SCORE_SCALE = 0.125
BLOCK = 256
MESH = pl.DeviceIdType.MESH
F32 = jnp.float32
BF16 = jnp.bfloat16
DP, MP = "dp", "mp"
INV_SQRT2 = 0.7071067811865476
INV_SQRT_2PI = 0.3989422804014327
NEG = -1e30

YN, NY, YD, ZYZ, YZZ = range(5)
HALVED = {ZYZ: (1, 0, 2), YZZ: (0, 1, 2)}
DOWN0, DOWN1, UP0, UP1, HEAD0, HEAD1, HEAD2, OUT = range(8)
PLANS = (YN, NY, YN, YN, YZZ, YZZ, YZZ, YZZ)
COLUMNS = (384, 384, 384, 384, 192, 192, 192, 192)
HELD = {YN: (8, 4, 2), NY: (8, 4, 2), YD: (8, 4), ZYZ: (8, 4, 2), YZZ: (8, 4, 2)}
ARRIVING = {YN: (4, 2, 2, 1), NY: (4, 4, 2, 1), YD: (4, 3), ZYZ: (4, 2, 1), YZZ: (4, 2, 1)}


POLLS = (
    ((DOWN0, 0), (DOWN1, 0)),
    (),
    (),
    ((UP0, 0), (DOWN0, 1)),
    ((DOWN1, 1),),
    (),
    ((UP1, 0), (DOWN0, 2)),
    ((UP0, 1),),
    ((DOWN1, 2), (UP1, 1), (HEAD0, 0)),
    ((UP0, 2), (DOWN0, 3), (HEAD1, 0), (UP1, 2), (HEAD2, 0), (OUT, 0)),
    ((UP0, 3), (DOWN1, 3), (HEAD0, 1), (HEAD1, 1), (HEAD2, 1), (OUT, 1), (UP1, 3)),
    ((HEAD0, 2), (HEAD1, 2), (HEAD2, 2), (OUT, 2)),
)


def packed_shape(piece, rows):
    columns = COLUMNS[piece]
    return (rows, columns) if columns == 384 else (rows // 2, 2 * columns)


def dot(left, right):
    return jnp.dot(left, right, preferred_element_type=F32)


def dot_nt(left, right):
    return lax.dot_general(left, right, (((1,), (1,)), ((), ())), preferred_element_type=F32)


def dot_tn(left, right):
    return lax.dot_general(left, right, (((0,), (0,)), ((), ())), preferred_element_type=F32)


def standardized(values):
    centered = values - jnp.mean(values, axis=-1, keepdims=True)
    variance = jnp.mean(centered * centered, axis=-1, keepdims=True)
    inverse = lax.rsqrt(variance + NORM_EPSILON)
    return centered * inverse, inverse


def norm_back(std_rows, inverse, gain, grad):
    scaled = gain * grad
    mean_scaled = jnp.mean(scaled, axis=-1, keepdims=True)
    mean_inner = jnp.mean(scaled * std_rows, axis=-1, keepdims=True)
    return inverse * (scaled - mean_scaled - std_rows * mean_inner)


def gelu_pair(values):
    bell = jnp.exp(-0.5 * (values * values))
    t = 1.0 / (1.0 + (0.3275911 * INV_SQRT2) * jnp.abs(values))
    tail = t * (0.127414796 + t * (-0.142248368 + t * (0.7107068705 + t * (-0.7265760135 + t * 0.5307027145)))) * bell
    phi = jnp.where(values >= 0.0, 1.0 - tail, tail)
    return values * phi, phi + values * (bell * INV_SQRT_2PI)


def column_sum(values):
    return jnp.sum(values, axis=0, keepdims=True)


def row_of(ref):
    return ref[...].astype(F32).reshape(1, -1)


def layer_kernel(names, dp_bits, *refs):
    r = types.SimpleNamespace(**dict(zip(names, refs)))
    of_pieces = iter(refs[len(names) :])
    grad_outs = [next(of_pieces) for _ in PLANS]
    grads = [next(of_pieces) for _ in PLANS]
    held = [[next(of_pieces) for _ in HELD[plan]] for plan in PLANS] if dp_bits else []
    arrived = [[next(of_pieces) for _ in ARRIVING[plan]] for plan in PLANS] if dp_bits else []
    rows, width = r.feats_hbm.shape
    heads = r.qw_hbm.shape[0]
    cols = heads * HD
    blocks = rows // BLOCK

    m = lax.axis_index(MP)
    c = m % 2
    x = m // 2
    cp = m + 1 - 2 * c
    xp = m + 2 - 4 * x

    def bit_of(bit):
        return (lax.axis_index(DP) // (1 << bit)) % 2

    def dp_peer(mask):
        peer = lax.axis_index(DP)
        for bit in range(3):
            if mask >> bit & 1:
                peer = peer + (1 << bit) * (1 - 2 * bit_of(bit))
        return peer

    def block_of(k):
        kx, kc = k // 2, k % 2
        return 2 * (x + kx - 2 * x * kx) + (c + kc - 2 * c * kc)

    def rows_at(start, size):
        return pl.ds(pl.multiple_of(start, size), size)

    own_heads = pl.ds(pl.multiple_of(m * cols, 64), cols)
    own = rows_at(m * BLOCK, BLOCK)

    first = dict(
        counts=(r.counts_hbm, r.counts), ow=(r.ow_hbm, r.ow.at[own_heads, :]), qw=(r.qw_hbm, r.wqkv.at[:, pl.ds(0, HD), :]),
        kw=(r.kw_hbm, r.wqkv.at[:, pl.ds(HD, HD), :]), vw=(r.vw_hbm, r.wqkv.at[:, pl.ds(2 * HD, HD), :]),
        gain_one=(r.gain_one_hbm, r.gain_one), shift_one=(r.shift_one_hbm, r.shift_one), q_bias=(r.q_bias_hbm, r.q_bias),
        v_bias=(r.v_bias_hbm, r.v_bias),
    )
    second = dict(
        o_bias=(r.o_bias_hbm, r.o_bias), gain_two=(r.gain_two_hbm, r.gain_two), shift_two=(r.shift_two_hbm, r.shift_two),
        up_bias=(r.up_bias_hbm, r.up_bias), down_bias=(r.down_bias_hbm, r.down_bias), og=(r.og_hbm, r.og),
        down=(r.down_hbm, r.down), up=(r.up_hbm, r.up),
    )
    loads = {**first, **second}
    load_index = {name: i for i, name in enumerate(loads)}

    def load(name):
        return pltpu.make_async_copy(*loads[name], r.load_sem.at[load_index[name]])

    def load_feats(i):
        here = rows_at(i * BLOCK, BLOCK)
        return pltpu.make_async_copy(r.feats_hbm.at[here, :], r.feats.at[here, :], r.load_sem.at[len(loads) + i])

    for name in first:
        load(name).start()
    for i in range(blocks):
        load_feats(i).start()
    for name in second:
        load(name).start()

    barrier = pltpu.get_barrier_semaphore()
    mp_peers = {1: cp, 2: xp, 3: block_of(3)}
    partners = [{MP: peer} for peer in mp_peers.values()] + [{DP: dp_peer(k)} for k in range(1, 1 << dp_bits)]
    for partner in partners:
        pl.semaphore_signal(barrier, inc=1, device_id=partner, device_id_type=MESH)

    def remote(index, source, target, partner):
        return pltpu.make_async_remote_copy(
            src_ref=source, dst_ref=target, send_sem=r.send_sem.at[index], recv_sem=r.recv_sem.at[index],
            device_id=partner, device_id_type=MESH,
        )

    OW, RL, BK, ML, IN, MG, SG, SD, MX = 0, 3, 6, 9, 13, 16, 19, 22, 29
    PIECE = MX + 12

    def ow_copy(kind):
        view = r.ow.at[pl.ds(pl.multiple_of((m, m, xp)[kind] * cols, 64), cols), :]
        return remote(OW + kind, view, view, {MP: (cp, xp, cp)[kind]})

    def mx_copy(kind, turn, place):
        owner = (m, m, xp)[kind]
        block = block_of(2 * turn + place if kind < 2 else 2 * (1 - turn) + place)
        view = r.mixed_t.at[block, pl.ds(pl.multiple_of(owner * cols, 64), cols), :]
        return remote(MX + (kind * 2 + turn) * 2 + place, view, view, {MP: (cp, xp, cp)[kind]})

    def rl_copy():
        return remote(RL, r.resid_low.at[c], r.resid_low.at[c], {MP: cp})

    def go_copy():
        return remote(RL + 1, r.go_tx, r.go_rx, {MP: xp})

    def rs_copy(base, step):
        send, receive = {BK: (r.bk_tx, r.bk_rx), ML: (r.ml_tx, r.ml_rx), IN: (r.bk_tx, r.in_rx)}[base]
        return remote(base + step, send.at[step], receive.at[step], {MP: (cp, xp, cp)[step]})

    def ml_x_copy(half):
        part = pl.ds(half * (BLOCK // 2), BLOCK // 2)
        return remote((ML + 1, ML + 3)[half], r.ml_tx.at[1, part], r.ml_rx.at[1, part], {MP: xp})

    def mg_copy(k):
        return remote(MG + k - 1, r.mg_tx.at[k - 1], r.mixed_grad_t.at[m], {MP: mp_peers[k]})

    def sg_copy(k):
        return remote(SG + k - 1, r.small_dp, r.sg_rx.at[k - 1], {MP: mp_peers[k]})

    def sd_copy(k):
        return remote(SD + k - 1, r.small_tx.at[dp_peer(k)], r.sd_rx.at[k - 1], {DP: dp_peer(k)})

    def store_piece(piece, tile, value):
        if not dp_bits:
            grads[piece][pl.ds(tile * 384, 384), :] = value
            return
        columns = COLUMNS[piece]
        weight = {YN: (4, 1, 2), YD: (4, 1, 2), NY: (1, 2, 4), ZYZ: (2, 4, 1), YZZ: (4, 2, 1)}[PLANS[piece]]
        for j in range(4):
            place = (j % 2) * weight[0] + (j // 2) * weight[1] + tile * weight[2]
            block = value[j * 96 : (j + 1) * 96].astype(BF16)
            if columns == 384:
                held[piece][0][place] = block
            else:
                held[piece][0][place, :, :columns] = block[:48]
                held[piece][0][place, :, columns:] = block[48:]

    y, z = bit_of(0), lax.axis_index(DP) // 2
    side, inner = z // 2, ((z + 1) // 2) % 2
    facing = side + inner - 2 * side * inner

    def part(ref, start, count):
        return ref.at[pl.ds(start, count)]

    def dp_remote(piece, stage, source, mask, target=None):
        target = arrived[piece][stage] if target is None else target
        return remote(PIECE + 4 * piece + stage, source, target, {DP: dp_peer(mask)})

    def dp_copies(piece, stage):
        plan, mine = PLANS[piece], held[piece]
        if plan in HALVED:
            bit = HALVED[plan][stage]
            count = 4 >> stage
            return [(None, lambda: dp_remote(piece, stage, part(mine[stage], (1 - bit_of(bit)) * count, count), 1 << bit))]
        if plan == YD and stage == 1:
            return [
                (None, lambda k=k: remote(PIECE + 4 * piece + k, mine[1].at[dp_peer(2 * k) // 2], arrived[piece][1].at[k - 1],
                                          {DP: dp_peer(2 * k)}))
                for k in (3, 2, 1)
            ]
        if stage == (3 if plan == NY else 0):
            count = 1 if plan == NY else 4
            source = mine[2] if plan == NY else mine[0]
            return [(None, lambda: dp_remote(piece, stage, part(source, (1 - y) * count, count), 1))]
        size = 2 if plan == NY else 1
        step = stage if plan == NY else stage - 1
        pair = mine[1 if plan == NY else 2]
        if step == 0:
            return [(None, lambda: dp_remote(piece, stage, part(mine[0 if plan == NY else 1], 2 * size * (1 - facing), 2 * size), 2))]
        if step == 1:
            return [(1, lambda: dp_remote(piece, stage, pair, 6))]
        place = (1 - z % 2) * size
        return [
            (1, lambda: dp_remote(piece, stage, part(arrived[piece][stage - 1], place, size), 2)),
            (0, lambda: dp_remote(piece, stage, part(pair, place, size), 2)),
        ]

    def each(piece, stage, action, only=None):
        for flag, make in dp_copies(piece, stage):
            if flag is None:
                action(make())
            elif only is None or only == flag:

                @pl.when(inner == flag)
                def _():
                    action(make())

    def start(copy):
        copy.start()

    def arrive(copy):
        copy.wait_recv()

    def leave(copy):
        copy.wait_send()

    def dp_start(*pieces):
        if dp_bits:
            for piece in pieces:
                each(piece, 0, start)

    def summed(first_ref, first_place, second_ref, second_place, count, target):
        for i in range(count):
            total = first_ref[first_place + i].astype(F32) + second_ref[second_place + i].astype(F32)
            if target is None:
                return total
            target[i] = total.astype(BF16)

    def dp_finish(stage, *pieces):
        for piece in pieces if dp_bits else ():
            plan, mine, came = PLANS[piece], held[piece], arrived[piece]
            if plan in HALVED:
                each(piece, stage, arrive)
                count = 4 >> stage
                kept = bit_of(HALVED[plan][stage]) * count
                if stage < 2:
                    summed(mine[stage], kept, came[stage], 0, count, mine[stage + 1])
                    each(piece, stage + 1, start)
                else:
                    grads[piece][...] = summed(mine[2], kept, came[2], 0, 1, None)
                continue
            if plan == YD and stage == 1:
                total = mine[1][z].astype(F32)
                each(piece, 1, arrive)
                for k in range(3):
                    total = total + came[1][k].astype(F32)
                grads[piece][...] = total
                continue
            if plan != NY and stage == 0:
                each(piece, 0, arrive)
                summed(mine[0], 4 * y, came[0], 0, 4, mine[1])
                each(piece, 1, start)
                continue
            if plan == NY and stage == 3:
                each(piece, 3, arrive)
                grads[piece][...] = summed(mine[2], y, came[3], 0, 1, None)
                continue
            size = 2 if plan == NY else 1
            step = stage if plan == NY else stage - 1
            pair = mine[1 if plan == NY else 2]
            if step == 0:
                each(piece, stage, arrive)
                summed(mine[0 if plan == NY else 1], 2 * size * facing, came[stage], 0, 2 * size, pair)
                each(piece, stage + 1, start, 1)
                each(piece, stage + 2, start, 0)
            elif step == 1:
                each(piece, stage, arrive, 1)
                each(piece, stage + 1, start, 1)
            else:
                arrive(dp_copies(piece, stage)[0][1]())
                place = (z % 2) * size
                for flag, source in ((1, came[stage - 1]), (0, pair)):

                    @pl.when(inner == flag)
                    def _():
                        if plan == NY:
                            summed(source, place, came[stage], 0, 2, mine[2])
                        else:
                            grads[piece][...] = summed(source, place, came[stage], 0, 1, None)

                if plan == NY:
                    each(piece, stage + 1, start)

    done = [(r.layer_out_v, r.layer_out), (r.feats_grad_v, r.feats_grad), (r.small_out_v, r.small_out)]
    done += list(zip(grads, grad_outs))

    def write_out(i):
        return pltpu.make_async_copy(*done[i], r.out_sem.at[i])

    def poll(point):
        for piece, stage in POLLS[point] if dp_bits else ():
            dp_finish(stage, piece)
            if stage == len(ARRIVING[PLANS[piece]]) - 1:
                write_out(3 + piece).start()

    pl.semaphore_wait(barrier, len(partners))
    load("ow").wait()
    ow_copy(1).start()
    ow_copy(0).start()
    for name in first:
        if name != "ow":
            load(name).wait()
    count = r.counts[0]
    gain_one, shift_one = row_of(r.gain_one), row_of(r.shift_one)
    q_bias = jnp.broadcast_to(row_of(r.q_bias), (128, cols)).T[:, :1]
    v_bias = jnp.broadcast_to(row_of(r.v_bias), (128, cols)).T[:, :1]
    lane = lax.broadcasted_iota(jnp.int32, (HD, BLOCK), 1)
    first_row = lax.broadcasted_iota(jnp.int32, (HD, BLOCK), 0) == 0
    one = jnp.where(first_row, 1.0, 0.0).astype(BF16)

    @pl.loop(0, blocks)
    def _(i):
        here = rows_at(i * BLOCK, BLOCK)
        load_feats(i).wait()
        std_rows, _ = standardized(r.feats[here, :].astype(F32))
        r.std_one[here, :] = std_rows.astype(BF16)
        normed = (std_rows * gain_one + shift_one).astype(BF16)
        r.normed[here, :] = normed
        projected = dot_nt(r.wqkv[...].reshape(3 * cols, width), normed)
        bias = jnp.where(jnp.logical_and(first_row, lane + i * BLOCK >= count), NEG, 0.0).astype(BF16)
        for h in range(heads):
            part = slice(h * HD, (h + 1) * HD)
            of_head = projected[3 * h * HD : 3 * (h + 1) * HD]
            query = ((of_head[:HD] + q_bias[part]).astype(BF16).astype(F32) * SCORE_SCALE).astype(BF16)
            keys = of_head[HD : 2 * HD].astype(BF16)
            values = (of_head[2 * HD :] + v_bias[part]).astype(BF16)
            r.query_t[i, h] = jnp.concatenate([query, one], axis=0)
            r.keys[h, here, :] = jnp.concatenate([keys, bias], axis=0).T
            r.values[h, here, :] = values.T
            r.keys_t[h, :, here] = keys
            r.values_t[h, :, here] = values

    @pl.loop(0, 2)
    def _(turn):
        units = [(block_of(2 * turn + place), h) for place in range(2) for h in range(heads)]
        scores = [dot(r.keys[h], r.query_t[block, h]) for block, h in units]
        for (block, h), score in zip(units, scores):
            peak = jnp.max(score, axis=0, keepdims=True)
            exped = jnp.exp(score - peak)
            total = jnp.sum(exped, axis=0, keepdims=True)
            exped = exped.astype(BF16)
            inverse = 1.0 / total
            r.exped[block, h] = exped
            r.inverse_total[block, h] = inverse
            mixed = dot(r.values_t[h], exped) * inverse
            r.mixed_t[block, pl.ds(pl.multiple_of(m * cols + h * HD, HD), HD), :] = mixed.astype(BF16)
        for place in range(2):
            mx_copy(1, turn, place).start()
            mx_copy(0, turn, place).start()

    for name in second:
        load(name).wait()
    slot = lax.broadcasted_iota(jnp.int32, (BLOCK, width), 0)
    r.key_acc[...] = jnp.zeros_like(r.key_acc)
    r.value_acc[...] = jnp.zeros_like(r.value_acc)

    @pl.loop(0, blocks)
    def _(i):
        here = rows_at(i * BLOCK, BLOCK)
        grad = r.og[here, :]
        grad = jnp.where(slot + i * BLOCK < count, grad.astype(F32), 0.0).astype(BF16)
        r.og[here, :] = grad
        r.hidden_grad[here, :] = dot_nt(grad, r.down[...])

    def mx_forward(turn):
        for place in range(2):
            mx_copy(1, turn, place).wait_recv()
            mx_copy(2, turn, place).start()

    def mx_arrive(kind, turn):
        for place in range(2):
            mx_copy(kind, turn, place).wait_recv()

    ow_copy(1).wait_recv()
    ow_copy(2).start()
    mx_forward(0)
    mx_arrive(0, 1)
    ow_copy(0).wait_recv()
    ow_copy(2).wait_recv()
    mx_arrive(2, 0)

    o_bias = row_of(r.o_bias)
    gain_two, shift_two = row_of(r.gain_two), row_of(r.shift_two)
    up_bias, down_bias = row_of(r.up_bias), row_of(r.down_bias)

    def feed_forward(pair, between):
        places = [rows_at(block_of(k) * BLOCK, BLOCK) for k in pair]
        attended = [dot_tn(r.mixed_t[block_of(k)], r.ow[...]) for k in pair]
        between()
        normed_two = []
        for k, here, value in zip(pair, places, attended):
            resid = r.feats[here, :].astype(F32) + (value + o_bias)
            std_rows, inverse = standardized(resid)
            if k == 0:
                r.resid[...] = resid
                r.std_two[...] = std_rows
                r.inverse_two[...] = inverse
            normed_two.append((std_rows * gain_two + shift_two).astype(BF16))
            r.normed_two[here, :] = normed_two[-1]
        pre_up = [dot(value, r.up[...]) + up_bias for value in normed_two]
        pre_grads = []
        for here, value in zip(places, pre_up):
            hidden, slope = gelu_pair(value)
            r.hidden[here, :] = hidden.astype(BF16)
            pre_grads.append((r.hidden_grad[here, :] * slope).astype(BF16))
            r.pre_grad[here, :] = pre_grads[-1]
        return pre_grads

    def feed_forward_out(k):
        return dot(r.hidden[rows_at(block_of(k) * BLOCK, BLOCK), :], r.down[...])

    pre_grads = feed_forward((3, 2), lambda: None)
    mx_forward(1)
    r.bk_tx[0] = dot_nt(pre_grads[0], r.up[...]).astype(BF16)
    rs_copy(BK, 0).start()
    r.back[...] = dot_nt(pre_grads[1], r.up[...])

    def send_back():
        rs_copy(BK, 0).wait_recv()
        r.bk_tx[1] = (r.back[...] + r.bk_rx[0].astype(F32)).astype(BF16)
        rs_copy(BK, 1).start()

    mx_arrive(0, 0)
    mx_arrive(2, 1)
    pre_grads = feed_forward((1, 0), send_back)

    def grad_tiles(left, right, pieces):
        right_all = right[...]

        @pl.loop(0, 2)
        def _(t):
            value = dot_tn(left[:, rows_at(t * 384, 384)], right_all)
            store_piece(pieces[0], t, value[:, :384])
            store_piece(pieces[1], t, value[:, 384:])

        dp_start(*pieces)

    grad_tiles(r.og, r.hidden, (DOWN0, DOWN1))
    grad_tiles(r.normed_two, r.pre_grad, (UP0, UP1))

    r.ml_tx[0] = feed_forward_out(3).astype(BF16)
    rs_copy(ML, 0).start()
    ml_x = feed_forward_out(2)
    r.bk_tx[2] = dot_nt(r.pre_grad[rows_at(block_of(1) * BLOCK, BLOCK), :], r.up[...]).astype(BF16)
    rs_copy(BK, 2).start()
    rs_copy(ML, 0).wait_recv()
    r.ml_tx[1] = (ml_x + r.ml_rx[0].astype(F32)).astype(BF16)
    ml_x_copy(0).start()
    r.back[...] = dot_nt(r.pre_grad[own, :], r.up[...])
    r.ml_tx[2] = feed_forward_out(1).astype(BF16)
    rs_copy(ML, 2).start()
    r.ml_own[...] = feed_forward_out(0)
    ones = jnp.ones((8, rows), BF16)
    r.small[6:7, :] = dot(ones, r.pre_grad[...])[:1]

    rs_copy(BK, 2).wait_recv()
    rs_copy(BK, 1).wait_recv()
    back = r.back[...] + r.bk_rx[2].astype(F32) + r.bk_rx[1].astype(F32)
    std_rows, inverse = r.std_two[...], r.inverse_two[...]
    own_grad = r.og[own, :].astype(F32)
    resid_grad = own_grad + norm_back(std_rows, inverse, gain_two, back)
    resid_low = resid_grad.astype(BF16)
    for k in (2, 3, 1):
        target_heads = r.ow[pl.ds(pl.multiple_of(mp_peers[k] * cols, 64), cols), :]
        r.mg_tx[k - 1] = dot_nt(target_heads, resid_low).astype(BF16)
        mg_copy(k).start()
    r.mixed_grad_t[m] = dot_nt(r.ow[own_heads, :], resid_low).astype(BF16)
    r.resid_grad[...] = resid_grad
    r.resid_low[c] = resid_low
    rl_copy().start()
    r.back[...] = back

    def attend_back(block):
        for h in range(heads):
            part = slice(h * HD, (h + 1) * HD)
            exped = r.exped[block, h]
            scaled = (r.mixed_grad_t[block, part, :].astype(F32) * r.inverse_total[block, h]).astype(BF16)
            mixed = r.mixed_t[block, pl.ds(pl.multiple_of(m * cols + h * HD, HD), HD), :]
            inner_product = column_sum(scaled.astype(F32) * mixed.astype(F32))
            prob_grad = dot(r.values[h], scaled)
            score_grad = (exped.astype(F32) * (prob_grad - inner_product)).astype(BF16)
            r.value_acc[h] += dot_nt(scaled, exped)
            r.key_acc[h] += dot_nt(r.query_t[block, h][:HD], score_grad)
            query_grad = dot(r.keys_t[h], score_grad) * SCORE_SCALE
            r.dqkv_t[3 * h * HD : (3 * h + 1) * HD, rows_at(block * BLOCK, BLOCK)] = query_grad.astype(BF16)

    def out_partial(head_rows):
        value = dot(r.mixed_t[m, head_rows, :], r.resid_low[c])
        return value + dot(r.mixed_t[cp, head_rows, :], r.resid_low[1 - c])

    @pl.loop(0, blocks)
    def _(i):
        @pl.when(i == 1)
        def _():
            poll(0)
            mg_copy(1).wait_recv()
            rl_copy().wait_recv()
            r.go_tx[...] = out_partial(pl.ds(pl.multiple_of(xp * cols, 64), cols)).astype(BF16)
            go_copy().start()
            ml_x_copy(1).start()

        @pl.when(i == 2)
        def _():
            poll(1)
            mg_copy(2).wait_recv()

        @pl.when(i == 3)
        def _():
            poll(2)
            mg_copy(3).wait_recv()

        attend_back(block_of(i))

    poll(3)

    for h in range(heads):
        row = 3 * h * HD
        r.dqkv_t[row + HD : row + 2 * HD, :] = r.key_acc[h].astype(BF16)
        r.dqkv_t[row + 2 * HD : row + 3 * HD, :] = r.value_acc[h].astype(BF16)
    value = dot(r.dqkv_t[...], r.normed[...])
    if dp_bits:
        value = value.astype(BF16)
    for t in range(2):
        for h in range(heads):
            store_piece(HEAD0 + h, t, value[h * cols : (h + 1) * cols, t * 384 : (t + 1) * 384].T)
    dp_start(HEAD0, HEAD1, HEAD2)
    poll(4)

    for step in range(3):
        rs_copy(BK, step).wait_send()
    r.gain_sum[...] = jnp.zeros_like(r.gain_sum)
    r.shift_sum[...] = jnp.zeros_like(r.shift_sum)

    def input_block(i):
        here = rows_at(block_of(3 - i) * BLOCK, BLOCK)
        part = dot_tn(r.dqkv_t[:, here], r.wqkv[...].reshape(3 * cols, width))

        @pl.when(i == 0)
        def _():
            r.bk_tx[0] = part.astype(BF16)
            rs_copy(IN, 0).start()

        @pl.when(i == 1)
        def _():
            rs_copy(IN, 0).wait_recv()
            r.bk_tx[1] = (part + r.in_rx[0].astype(F32)).astype(BF16)
            rs_copy(IN, 1).start()

        @pl.when(i == 2)
        def _():
            r.bk_tx[2] = part.astype(BF16)
            rs_copy(IN, 2).start()

        @pl.when(i == 3)
        def _():
            r.back[...] = part

        r.gain_sum[...] += column_sum(part * r.std_one[here, :].astype(F32))
        r.shift_sum[...] += column_sum(part)

    @pl.loop(0, 2)
    def _(i):
        input_block(i)

    poll(5)

    go_copy().wait_recv()
    value = out_partial(own_heads) + r.go_rx[...].astype(F32)
    for t in range(2):
        store_piece(OUT, t, value[:, t * 384 : (t + 1) * 384].T)
    dp_start(OUT)
    poll(6)

    r.small[2:3, :] = column_sum(r.resid_low[c].astype(F32))
    r.small[3:4, :] = column_sum(r.back[...] * r.std_two[...])
    r.small[4:5, :] = column_sum(r.back[...])
    r.small[5:6, :] = column_sum(r.og[own, :].astype(F32))

    @pl.loop(0, 2)
    def _(i):
        input_block(i + 2)

    poll(7)

    r.small[0:1, :] = r.gain_sum[...]
    r.small[1:2, :] = r.shift_sum[...]
    bias_sums = dot_nt(jnp.ones((8, rows), BF16), r.dqkv_t[...])[:1]
    q_sums = jnp.concatenate([bias_sums[:, 3 * h * HD : (3 * h + 1) * HD] for h in range(heads)], axis=1)
    v_sums = jnp.concatenate([bias_sums[:, (3 * h + 2) * HD : 3 * (h + 1) * HD] for h in range(heads)], axis=1)
    if dp_bits:
        dp_size = 1 << dp_bits
        share, head_share = width // dp_size, cols // dp_size
        blank = jnp.zeros((1, 128 - 2 * head_share), F32)
        for peer in range(dp_size):
            r.small_tx[peer, 0:7, :share] = r.small[0:7, peer * share : (peer + 1) * share]
            of_peer = slice(peer * head_share, (peer + 1) * head_share)
            r.small_tx[peer, 7:8, :] = jnp.concatenate([q_sums[:, of_peer], v_sums[:, of_peer], blank], axis=1)
        for k in range(1, dp_size):
            sd_copy(k).start()
    else:
        r.small[7:8, :] = jnp.concatenate([q_sums, v_sums, jnp.zeros((1, width - 2 * cols), F32)], axis=1)

    poll(8)
    ml_x_copy(0).wait_recv()
    ml_x_copy(1).wait_recv()
    rs_copy(ML, 2).wait_recv()
    mlp = r.ml_own[...] + r.ml_rx[2].astype(F32) + r.ml_rx[1].astype(F32)
    r.layer_out_v[...] = (r.resid[...] + (mlp + down_bias)).astype(BF16)
    write_out(0).start()
    std_rows, inverse = standardized(r.feats[own, :].astype(F32))
    poll(9)

    if dp_bits:
        total = r.small_tx[lax.axis_index(DP)]
        for k in range(1, 1 << dp_bits):
            sd_copy(k).wait_recv()
            total = total + r.sd_rx[k - 1]
        r.small_dp[...] = total
    else:
        r.small_dp[...] = r.small[...]
    for k in mp_peers:
        sg_copy(k).start()

    poll(10)
    rs_copy(IN, 2).wait_recv()
    rs_copy(IN, 1).wait_recv()
    back = r.back[...] + r.in_rx[2].astype(F32) + r.in_rx[1].astype(F32)
    r.feats_grad_v[...] = (r.resid_grad[...] + norm_back(std_rows, inverse, gain_one, back)).astype(BF16)
    write_out(1).start()

    total = r.small_dp[...]
    for k in mp_peers:
        sg_copy(k).wait_recv()
        of_peer = r.sg_rx[k - 1]
        total = total + jnp.where(lax.broadcasted_iota(jnp.int32, of_peer.shape, 0) < 6, of_peer, 0.0)
    r.small_out_v[...] = total
    write_out(2).start()
    poll(11)
    if not dp_bits:
        for piece in range(len(PLANS)):
            write_out(3 + piece).start()

    for i in range(len(done)):
        write_out(i).wait()
    for kind in range(3):
        ow_copy(kind).wait_send()
        rs_copy(IN, kind).wait_send()
        for turn in range(2):
            for place in range(2):
                mx_copy(kind, turn, place).wait_send()
    rl_copy().wait_send()
    go_copy().wait_send()
    rs_copy(ML, 0).wait_send()
    rs_copy(ML, 2).wait_send()
    ml_x_copy(0).wait_send()
    ml_x_copy(1).wait_send()
    for k in mp_peers:
        mg_copy(k).wait_send()
        sg_copy(k).wait_send()
    if dp_bits:
        for k in range(1, 1 << dp_bits):
            sd_copy(k).wait_send()
        for piece, plan in enumerate(PLANS):
            for stage in range(len(ARRIVING[plan])):
                each(piece, stage, leave)


def finish_kernel(names, *refs):
    r = types.SimpleNamespace(**dict(zip(names, refs)))
    grads = refs[len(names) :]
    shard = r.up.shape[0]
    unpacked = (r.head0, r.head1, r.head2, r.o)
    incoming = [
        (r.small_out, r.small), (r.layer_out, r.layer), (r.feats_grad, r.feats), *zip(grads[HEAD0:], unpacked),
        (grads[UP0], r.up.at[:, pl.ds(0, 384)]), (grads[UP1], r.up.at[:, pl.ds(384, 384)]),
        (grads[DOWN0], r.down.at[:, pl.ds(0, 384)]), (grads[DOWN1], r.down.at[:, pl.ds(384, 384)]),
    ]
    outgoing = [
        (r.layer, r.out_layer), (r.feats, r.out_feats), (r.up, r.out_up), (r.down, r.out_down), (r.q, r.out_q),
        (r.k, r.out_k), (r.v, r.out_v), (r.o_t, r.out_o), (r.up_bias, r.out_up_bias),
    ]
    vectors = (r.out_gain_one, r.out_shift_one, r.out_o_bias, r.out_gain_two, r.out_shift_two, r.out_down_bias, r.out_q_bias,
               r.out_v_bias)
    outgoing += [(r.pieces.at[i], target) for i, target in enumerate(vectors)]

    def take(i):
        return pltpu.make_async_copy(*incoming[i], r.in_sem.at[i])

    def give(i):
        return pltpu.make_async_copy(*outgoing[i], r.out_sem.at[i])

    for i in range(len(incoming)):
        take(i).start()
    take(0).wait()
    m = lax.axis_index(MP)
    small = r.small[...]
    piece = r.out_gain_one.shape[0]
    mine = pltpu.roll(small, (128 - m * piece) % 128, 1)
    for i in range(6):
        r.pieces[i] = mine[i, :piece]
    r.pieces[6] = small[7, :piece]
    r.pieces[7] = small[7, piece : 2 * piece]
    r.up_bias[...] = small[6, :shard]
    for i in range(8, len(outgoing)):
        give(i).start()
    for i in (1, 2):
        take(i).wait()
        give(i - 1).start()
    for i in range(3, 7):
        take(i).wait()
    heads = [jnp.concatenate([ref[:, :192], ref[:, 192:]], axis=0) for ref in unpacked]
    for i, target in enumerate((r.q, r.k, r.v)):
        target[...] = jnp.concatenate([value[:, i * HD : (i + 1) * HD] for value in heads[:3]], axis=1)
        give(4 + i).start()
    r.o_t[...] = heads[3].T
    give(7).start()
    for i in range(7, 11):
        take(i).wait()
        if i % 2 == 0:
            give((i - 4) // 2).start()
    for i in range(len(outgoing)):
        give(i).wait()


def layer_call(dp_size, clip_feats, counts, gain_one, shift_one, q_weight, k_weight, v_weight, q_bias, v_bias, o_weight,
               o_bias, gain_two, shift_two, up_weight, up_bias, down_weight, down_bias, out_grad):
    rows, width = clip_feats.shape
    cols = q_weight.shape[1]
    heads = cols // HD
    hidden_cols = up_weight.shape[1]
    dp_bits = 3 if dp_size == 8 else 0
    vmem = pl.BlockSpec(memory_space=pltpu.VMEM)
    anywhere = pl.BlockSpec(memory_space=pl.ANY)
    by_head = (heads, HD, width)
    inputs = dict(
        gain_one_hbm=(gain_one, anywhere), shift_one_hbm=(shift_one, anywhere), q_bias_hbm=(q_bias, anywhere),
        v_bias_hbm=(v_bias, anywhere), o_bias_hbm=(o_bias, anywhere), gain_two_hbm=(gain_two, anywhere),
        shift_two_hbm=(shift_two, anywhere), up_bias_hbm=(up_bias, anywhere),
        down_bias_hbm=(down_bias, anywhere), counts_hbm=(counts, anywhere),
        feats_hbm=(clip_feats, anywhere), qw_hbm=(q_weight.T.reshape(by_head), anywhere),
        kw_hbm=(k_weight.T.reshape(by_head), anywhere), vw_hbm=(v_weight.T.reshape(by_head), anywhere),
        ow_hbm=(o_weight, anywhere), up_hbm=(up_weight, anywhere),
        down_hbm=(down_weight, anywhere), og_hbm=(out_grad, anywhere),
    )
    shard = width // dp_size if dp_bits else width
    small_shape = (8, 128) if dp_bits else (8, width)
    outputs = dict(layer_out=((BLOCK, width), BF16), feats_grad=((BLOCK, width), BF16), small_out=(small_shape, F32))
    grads = [(packed_shape(i, shard) if dp_bits else (width, COLUMNS[i]), F32) for i in range(len(PLANS))]
    piece = (BLOCK, width)
    scratch = dict(
        gain_one=((width,), BF16), shift_one=((width,), BF16), q_bias=((cols,), BF16), v_bias=((cols,), BF16),
        o_bias=((width,), BF16), gain_two=((width,), BF16), shift_two=((width,), BF16),
        up_bias=((hidden_cols,), BF16), down_bias=((width,), BF16),
        feats=((rows, width), BF16), wqkv=((heads, 3 * HD, width), BF16), ow=((width, width), BF16),
        og=((rows, width), BF16), down=((hidden_cols, width), BF16), up=((width, hidden_cols), BF16),
        normed=((rows, width), BF16), std_one=((rows, width), BF16),
        query_t=((rows // BLOCK, heads, 2 * HD, BLOCK), BF16), keys=((heads, rows, 2 * HD), BF16), values=((heads, rows, HD), BF16),
        keys_t=((heads, HD, rows), BF16), values_t=((heads, HD, rows), BF16), mixed_t=((rows // BLOCK, width, BLOCK), BF16),
        exped=((rows // BLOCK, heads, rows, BLOCK), BF16), inverse_total=((rows // BLOCK, heads, 1, BLOCK), F32), hidden_grad=((rows, hidden_cols), F32), resid=(piece, F32),
        normed_two=((rows, width), BF16), hidden=((rows, hidden_cols), BF16), pre_grad=((rows, hidden_cols), BF16),
        back=(piece, F32), resid_grad=(piece, F32),
        resid_low=((2,) + piece, BF16), go_tx=((cols, width), BF16), go_rx=((cols, width), BF16), std_two=(piece, F32), inverse_two=((BLOCK, 1), F32), ml_own=(piece, F32),
        bk_tx=((3,) + piece, BF16), bk_rx=((3,) + piece, BF16), ml_tx=((3,) + piece, BF16),
        ml_rx=((3,) + piece, BF16), in_rx=((3,) + piece, BF16),
        mg_tx=((3, cols, BLOCK), BF16), mixed_grad_t=((rows // BLOCK, cols, BLOCK), BF16),
        key_acc=((heads, HD, rows), F32), value_acc=((heads, HD, rows), F32), dqkv_t=((3 * cols, rows), BF16),
        gain_sum=((1, width), F32), shift_sum=((1, width), F32),
        small=((8, width), F32), small_dp=(small_shape, F32), sg_rx=((3,) + small_shape, F32),
    )
    scratch.update({name + "_v": spec for name, spec in outputs.items()})
    of_pieces = list(grads)
    if dp_bits:
        scratch.update(
            small_tx=((dp_size,) + small_shape, F32), sd_rx=((dp_size - 1,) + small_shape, F32)
        )
        for table in (HELD, ARRIVING):
            for i, plan in enumerate(PLANS):
                of_pieces += [((count,) + packed_shape(i, shard), BF16) for count in table[plan]]
    copies = 29 + 12 + 4 * len(PLANS)
    scalars = dict(
        counts=pltpu.SMEM((1,), jnp.int32), load_sem=pltpu.SemaphoreType.DMA((17 + rows // BLOCK,)),
        out_sem=pltpu.SemaphoreType.DMA((len(outputs) + len(grads),)), send_sem=pltpu.SemaphoreType.DMA((copies,)),
        recv_sem=pltpu.SemaphoreType.DMA((copies,)),
    )
    names = list(inputs) + list(outputs)
    kernel_names = [*inputs, *outputs, *scratch, *scalars]

    def kernel(*refs):
        refs = list(refs)
        grad_refs = refs[len(names) : len(names) + len(grads)]
        rest = refs[len(names) + len(grads) :]
        named = len(scratch) + len(scalars)
        layer_kernel(kernel_names, dp_bits, *refs[: len(names)], *rest[:named], *grad_refs, *rest[named:])

    results = pl.pallas_call(
        kernel,
        out_shape=[jax.ShapeDtypeStruct(*spec) for spec in [*outputs.values(), *grads]],
        in_specs=[spec for _, spec in inputs.values()],
        out_specs=[anywhere] * (len(outputs) + len(grads)),
        scratch_shapes=[pltpu.VMEM(*spec) for spec in scratch.values()] + list(scalars.values())
        + [pltpu.VMEM(*spec) for spec in of_pieces],
        compiler_params=pltpu.CompilerParams(collective_id=0, has_side_effects=True, vmem_limit_bytes=67043328),
        name="layer",
    )(*[value for value, _ in inputs.values()])
    return dict(zip(outputs, results)), results[len(outputs) :]


def finish_call(out, grads, cols, hidden_cols):
    shard, width = COLUMNS[UP0] // 4, out["layer_out"].shape[1]
    rows = ((BLOCK, width), BF16)
    small = ((shard // 4,), F32)
    head = ((shard, cols), F32)
    shapes = dict(
        out_layer=rows, out_feats=rows, out_gain_one=small, out_shift_one=small, out_q=head, out_k=head, out_v=head,
        out_q_bias=small, out_v_bias=small, out_o=((cols, shard), F32), out_o_bias=small, out_gain_two=small,
        out_shift_two=small, out_up=((shard, hidden_cols), F32), out_up_bias=((shard,), F32),
        out_down=((shard, hidden_cols), F32), out_down_bias=small,
    )
    packed = (packed_shape(OUT, shard), F32)
    scratch = dict(
        small=((8, 128), F32), layer=rows, feats=rows, head0=packed, head1=packed, head2=packed, o=packed,
        up=((shard, hidden_cols), F32), down=((shard, hidden_cols), F32), q=head, k=head, v=head, o_t=((cols, shard), F32),
        up_bias=((shard,), F32), pieces=((8, shard // 4), F32),
    )
    sems = dict(in_sem=pltpu.SemaphoreType.DMA((11,)), out_sem=pltpu.SemaphoreType.DMA((17,)))
    names = [*out, *shapes, *scratch, *sems]

    def kernel(*refs):
        count = len(out) + len(grads)
        finish_kernel(names, *refs[: len(out)], *refs[count:], *refs[len(out) : count])

    anywhere = pl.BlockSpec(memory_space=pl.ANY)
    results = pl.pallas_call(
        kernel,
        out_shape=[jax.ShapeDtypeStruct(*spec) for spec in shapes.values()],
        in_specs=[anywhere] * (len(out) + len(grads)),
        out_specs=[anywhere] * len(shapes),
        scratch_shapes=[pltpu.VMEM(*spec) for spec in scratch.values()] + list(sems.values()),
        name="finish",
    )(*out.values(), *grads)
    return (*results[:15], results[15].T, results[16])


def shards(dp_size, *args):
    out, grads = layer_call(dp_size, *args)
    cols, hidden_cols = args[4].shape[1], args[13].shape[1]
    if dp_size == 8:
        return finish_call(out, grads, cols, hidden_cols)

    def over(value, dim):
        return lax.psum_scatter(value, DP, scatter_dimension=dim, tiled=True)

    small = lax.psum(out["small_out"], DP)
    width = small.shape[1]
    d, m = lax.axis_index(DP), lax.axis_index(MP)
    piece = width // (dp_size * 4)
    group = [lax.dynamic_slice(small, (i, (d * 4 + m) * piece), (1, piece)).reshape(piece) for i in range(6)]
    up_piece = hidden_cols // dp_size
    head_piece = cols // dp_size
    up_bias = lax.dynamic_slice(small, (6, d * up_piece), (1, up_piece)).reshape(up_piece)
    q_bias = lax.dynamic_slice(small, (7, d * head_piece), (1, head_piece)).reshape(head_piece)
    v_bias = lax.dynamic_slice(small, (7, cols + d * head_piece), (1, head_piece)).reshape(head_piece)
    heads = grads[HEAD0 : HEAD2 + 1]
    q_grad, k_grad, v_grad = (
        jnp.concatenate([value[:, i * HD : (i + 1) * HD] for value in heads], axis=1) for i in range(3)
    )
    up_grad = jnp.concatenate([grads[UP0], grads[UP1]], axis=1)
    down_grad = jnp.concatenate([grads[DOWN0], grads[DOWN1]], axis=1)
    return (
        out["layer_out"], out["feats_grad"], group[0], group[1], over(q_grad, 0), over(k_grad, 0), over(v_grad, 0),
        q_bias, v_bias, over(grads[OUT].T, 1), group[2], group[3], group[4], over(up_grad, 0), up_bias,
        over(down_grad.T, 1), group[5],
    )


def solution(mesh):
    placed = (
        P(DP, None), P(DP), P(), P(), P(None, MP), P(None, MP), P(None, MP), P(MP), P(MP), P(MP, None),
        P(), P(), P(), P(None, MP), P(MP), P(MP, None), P(), P(DP, None),
    )
    return jax.shard_map(
        functools.partial(shards, mesh.shape[DP]),
        mesh=mesh,
        in_specs=placed,
        out_specs=(
            P((DP, MP), None), P((DP, MP), None), P((DP, MP)), P((DP, MP)), P(DP, MP), P(DP, MP),
            P(DP, MP), P((MP, DP)), P((MP, DP)), P(MP, DP), P((DP, MP)), P((DP, MP)),
            P((DP, MP)), P(DP, MP), P((MP, DP)), P(MP, DP), P((DP, MP)),
        ),
        check_vma=False,
    )
```

```python
import functools
import types

import jax
import jax.numpy as jnp
from jax import lax
from jax.experimental import pallas as pl
from jax.experimental.pallas import tpu as pltpu
from jax.sharding import PartitionSpec as P

HD = 64
NORM_EPSILON = 1e-06
SCORE_SCALE = 0.125
BLOCK = 256
MESH = pl.DeviceIdType.MESH
F32 = jnp.float32
BF16 = jnp.bfloat16
DP, MP = "dp", "mp"
INV_SQRT2 = 0.7071067811865476
INV_SQRT_2PI = 0.3989422804014327
NEG = -1e30

YN, NY, YD, ZYZ, YZZ = range(5)
HALVED = {ZYZ: (1, 0, 2), YZZ: (0, 1, 2)}
DOWN0, DOWN1, UP0, UP1, HEAD0, HEAD1, HEAD2, OUT = range(8)
PLANS = (YN, NY, YN, YN, YZZ, YZZ, YZZ, YZZ)
COLUMNS = (384, 384, 384, 384, 192, 192, 192, 192)
HELD = {YN: (8, 4, 2), NY: (8, 4, 2), YD: (8, 4), ZYZ: (8, 4, 2), YZZ: (8, 4, 2)}
ARRIVING = {YN: (4, 2, 2, 1), NY: (4, 4, 2, 1), YD: (4, 3), ZYZ: (4, 2, 1), YZZ: (4, 2, 1)}


POLLS = (
    ((DOWN0, 0), (DOWN1, 0)),
    (),
    ((UP0, 0),),
    ((DOWN0, 1),),
    ((DOWN1, 1),),
    ((UP1, 0),),
    ((DOWN0, 2), (UP0, 1)),
    (),
    ((HEAD0, 0), (DOWN1, 2), (UP1, 1)),
    ((HEAD1, 0), (UP0, 2), (DOWN0, 3), (HEAD0, 1), (HEAD2, 0), (UP1, 2)),
    ((HEAD1, 1), (OUT, 0), (UP0, 3), (DOWN1, 3), (HEAD2, 1), (UP1, 3), (OUT, 1)),
    ((HEAD0, 2), (HEAD1, 2), (HEAD2, 2), (OUT, 2)),
)


def packed_shape(piece, rows):
    columns = COLUMNS[piece]
    return (rows, columns) if columns == 384 else (rows // 2, 2 * columns)


def dot(left, right):
    return jnp.dot(left, right, preferred_element_type=F32)


def dot_nt(left, right):
    return lax.dot_general(left, right, (((1,), (1,)), ((), ())), preferred_element_type=F32)


def dot_tn(left, right):
    return lax.dot_general(left, right, (((0,), (0,)), ((), ())), preferred_element_type=F32)


def standardized(values):
    centered = values - jnp.mean(values, axis=-1, keepdims=True)
    variance = jnp.mean(centered * centered, axis=-1, keepdims=True)
    inverse = lax.rsqrt(variance + NORM_EPSILON)
    return centered * inverse, inverse


def norm_back(std_rows, inverse, gain, grad):
    scaled = gain * grad
    mean_scaled = jnp.mean(scaled, axis=-1, keepdims=True)
    mean_inner = jnp.mean(scaled * std_rows, axis=-1, keepdims=True)
    return inverse * (scaled - mean_scaled - std_rows * mean_inner)


def gelu_pair(values):
    bell = jnp.exp(-0.5 * (values * values))
    t = 1.0 / (1.0 + (0.3275911 * INV_SQRT2) * jnp.abs(values))
    tail = t * (0.127414796 + t * (-0.142248368 + t * (0.7107068705 + t * (-0.7265760135 + t * 0.5307027145)))) * bell
    phi = jnp.where(values >= 0.0, 1.0 - tail, tail)
    return values * phi, phi + values * (bell * INV_SQRT_2PI)


def column_sum(values):
    return jnp.sum(values, axis=0, keepdims=True)


def row_of(ref):
    return ref[...].astype(F32).reshape(1, -1)


def layer_kernel(names, dp_bits, *refs):
    r = types.SimpleNamespace(**dict(zip(names, refs)))
    of_pieces = iter(refs[len(names) :])
    grad_outs = [next(of_pieces) for _ in PLANS]
    grads = [next(of_pieces) for _ in PLANS]
    held = [[next(of_pieces) for _ in HELD[plan]] for plan in PLANS] if dp_bits else []
    arrived = [[next(of_pieces) for _ in ARRIVING[plan]] for plan in PLANS] if dp_bits else []
    rows, width = r.feats_hbm.shape
    heads = r.qw_hbm.shape[0]
    cols = heads * HD
    blocks = rows // BLOCK

    m = lax.axis_index(MP)
    c = m % 2
    x = m // 2
    cp = m + 1 - 2 * c
    xp = m + 2 - 4 * x

    def bit_of(bit):
        return (lax.axis_index(DP) // (1 << bit)) % 2

    def dp_peer(mask):
        peer = lax.axis_index(DP)
        for bit in range(3):
            if mask >> bit & 1:
                peer = peer + (1 << bit) * (1 - 2 * bit_of(bit))
        return peer

    def block_of(k):
        kx, kc = k // 2, k % 2
        return 2 * (x + kx - 2 * x * kx) + (c + kc - 2 * c * kc)

    def rows_at(start, size):
        return pl.ds(pl.multiple_of(start, size), size)

    own_heads = pl.ds(pl.multiple_of(m * cols, 64), cols)
    own = rows_at(m * BLOCK, BLOCK)

    first = dict(
        counts=(r.counts_hbm, r.counts), ow=(r.ow_hbm, r.ow.at[own_heads, :]), qw=(r.qw_hbm, r.wqkv.at[:, pl.ds(0, HD), :]),
        kw=(r.kw_hbm, r.wqkv.at[:, pl.ds(HD, HD), :]), vw=(r.vw_hbm, r.wqkv.at[:, pl.ds(2 * HD, HD), :]),
        gain_one=(r.gain_one_hbm, r.gain_one), shift_one=(r.shift_one_hbm, r.shift_one), q_bias=(r.q_bias_hbm, r.q_bias),
        v_bias=(r.v_bias_hbm, r.v_bias),
    )
    second = dict(
        o_bias=(r.o_bias_hbm, r.o_bias), gain_two=(r.gain_two_hbm, r.gain_two), shift_two=(r.shift_two_hbm, r.shift_two),
        up_bias=(r.up_bias_hbm, r.up_bias), down_bias=(r.down_bias_hbm, r.down_bias), og=(r.og_hbm, r.og),
        down=(r.down_hbm, r.down), up=(r.up_hbm, r.up),
    )
    loads = {**first, **second}
    load_index = {name: i for i, name in enumerate(loads)}

    def load(name):
        return pltpu.make_async_copy(*loads[name], r.load_sem.at[load_index[name]])

    def load_feats(i):
        here = rows_at(i * BLOCK, BLOCK)
        return pltpu.make_async_copy(r.feats_hbm.at[here, :], r.feats.at[here, :], r.load_sem.at[len(loads) + i])

    for name in first:
        load(name).start()
    for i in range(blocks):
        load_feats(i).start()
    for name in second:
        load(name).start()

    barrier = pltpu.get_barrier_semaphore()
    mp_peers = {1: cp, 2: xp, 3: block_of(3)}
    partners = [{MP: peer} for peer in mp_peers.values()] + [{DP: dp_peer(k)} for k in range(1, 1 << dp_bits)]
    for partner in partners:
        pl.semaphore_signal(barrier, inc=1, device_id=partner, device_id_type=MESH)

    def remote(index, source, target, partner):
        return pltpu.make_async_remote_copy(
            src_ref=source, dst_ref=target, send_sem=r.send_sem.at[index], recv_sem=r.recv_sem.at[index],
            device_id=partner, device_id_type=MESH,
        )

    OW, RL, BK, ML, IN, MG, SG, SD, MX = 0, 3, 6, 9, 13, 16, 19, 22, 29
    PIECE = MX + 12

    def ow_copy(kind):
        view = r.ow.at[pl.ds(pl.multiple_of((m, m, xp)[kind] * cols, 64), cols), :]
        return remote(OW + kind, view, view, {MP: (cp, xp, cp)[kind]})

    def mx_copy(kind, turn, place):
        owner = (m, m, xp)[kind]
        block = block_of(2 * turn + place if kind < 2 else 2 * (1 - turn) + place)
        view = r.mixed_t.at[block, pl.ds(pl.multiple_of(owner * cols, 64), cols), :]
        return remote(MX + (kind * 2 + turn) * 2 + place, view, view, {MP: (cp, xp, cp)[kind]})

    def rl_copy():
        return remote(RL, r.resid_low.at[c], r.resid_low.at[c], {MP: cp})

    def go_copy():
        return remote(RL + 1, r.go_tx, r.go_rx, {MP: xp})

    def rs_copy(base, step):
        send, receive = {BK: (r.bk_tx, r.bk_rx), ML: (r.ml_tx, r.ml_rx), IN: (r.bk_tx, r.in_rx)}[base]
        return remote(base + step, send.at[step], receive.at[step], {MP: (cp, xp, cp)[step]})

    def mg_copy(k):
        return remote(MG + k - 1, r.mg_tx.at[k - 1], r.mixed_grad_t.at[m], {MP: mp_peers[k]})

    def sg_copy(k):
        return remote(SG + k - 1, r.small_dp, r.sg_rx.at[k - 1], {MP: mp_peers[k]})

    def sd_copy(k):
        return remote(SD + k - 1, r.small_tx.at[dp_peer(k)], r.sd_rx.at[k - 1], {DP: dp_peer(k)})

    def store_piece(piece, tile, value):
        if not dp_bits:
            grads[piece][pl.ds(tile * 384, 384), :] = value
            return
        columns = COLUMNS[piece]
        weight = {YN: (4, 1, 2), YD: (4, 1, 2), NY: (1, 2, 4), ZYZ: (2, 4, 1), YZZ: (4, 2, 1)}[PLANS[piece]]
        for j in range(4):
            place = (j % 2) * weight[0] + (j // 2) * weight[1] + tile * weight[2]
            block = value[j * 96 : (j + 1) * 96].astype(BF16)
            if columns == 384:
                held[piece][0][place] = block
            else:
                held[piece][0][place, :, :columns] = block[:48]
                held[piece][0][place, :, columns:] = block[48:]

    y, z = bit_of(0), lax.axis_index(DP) // 2
    side, inner = z // 2, ((z + 1) // 2) % 2
    facing = side + inner - 2 * side * inner

    def part(ref, start, count):
        return ref.at[pl.ds(start, count)]

    def dp_remote(piece, stage, source, mask, target=None):
        target = arrived[piece][stage] if target is None else target
        return remote(PIECE + 4 * piece + stage, source, target, {DP: dp_peer(mask)})

    def dp_copies(piece, stage):
        plan, mine = PLANS[piece], held[piece]
        if plan in HALVED:
            bit = HALVED[plan][stage]
            count = 4 >> stage
            return [(None, lambda: dp_remote(piece, stage, part(mine[stage], (1 - bit_of(bit)) * count, count), 1 << bit))]
        if plan == YD and stage == 1:
            return [
                (None, lambda k=k: remote(PIECE + 4 * piece + k, mine[1].at[dp_peer(2 * k) // 2], arrived[piece][1].at[k - 1],
                                          {DP: dp_peer(2 * k)}))
                for k in (3, 2, 1)
            ]
        if stage == (3 if plan == NY else 0):
            count = 1 if plan == NY else 4
            source = mine[2] if plan == NY else mine[0]
            return [(None, lambda: dp_remote(piece, stage, part(source, (1 - y) * count, count), 1))]
        size = 2 if plan == NY else 1
        step = stage if plan == NY else stage - 1
        pair = mine[1 if plan == NY else 2]
        if step == 0:
            return [(None, lambda: dp_remote(piece, stage, part(mine[0 if plan == NY else 1], 2 * size * (1 - facing), 2 * size), 2))]
        if step == 1:
            return [(1, lambda: dp_remote(piece, stage, pair, 6))]
        place = (1 - z % 2) * size
        return [
            (1, lambda: dp_remote(piece, stage, part(arrived[piece][stage - 1], place, size), 2)),
            (0, lambda: dp_remote(piece, stage, part(pair, place, size), 2)),
        ]

    def each(piece, stage, action, only=None):
        for flag, make in dp_copies(piece, stage):
            if flag is None:
                action(make())
            elif only is None or only == flag:

                @pl.when(inner == flag)
                def _():
                    action(make())

    def start(copy):
        copy.start()

    def arrive(copy):
        copy.wait_recv()

    def leave(copy):
        copy.wait_send()

    def dp_start(*pieces):
        if dp_bits:
            for piece in pieces:
                each(piece, 0, start)

    def summed(first_ref, first_place, second_ref, second_place, count, target):
        for i in range(count):
            total = first_ref[first_place + i].astype(F32) + second_ref[second_place + i].astype(F32)
            if target is None:
                return total
            target[i] = total.astype(BF16)

    def dp_finish(stage, *pieces):
        for piece in pieces if dp_bits else ():
            plan, mine, came = PLANS[piece], held[piece], arrived[piece]
            if plan in HALVED:
                each(piece, stage, arrive)
                count = 4 >> stage
                kept = bit_of(HALVED[plan][stage]) * count
                if stage < 2:
                    summed(mine[stage], kept, came[stage], 0, count, mine[stage + 1])
                    each(piece, stage + 1, start)
                else:
                    grads[piece][...] = summed(mine[2], kept, came[2], 0, 1, None)
                continue
            if plan == YD and stage == 1:
                total = mine[1][z].astype(F32)
                each(piece, 1, arrive)
                for k in range(3):
                    total = total + came[1][k].astype(F32)
                grads[piece][...] = total
                continue
            if plan != NY and stage == 0:
                each(piece, 0, arrive)
                summed(mine[0], 4 * y, came[0], 0, 4, mine[1])
                each(piece, 1, start)
                continue
            if plan == NY and stage == 3:
                each(piece, 3, arrive)
                grads[piece][...] = summed(mine[2], y, came[3], 0, 1, None)
                continue
            size = 2 if plan == NY else 1
            step = stage if plan == NY else stage - 1
            pair = mine[1 if plan == NY else 2]
            if step == 0:
                each(piece, stage, arrive)
                summed(mine[0 if plan == NY else 1], 2 * size * facing, came[stage], 0, 2 * size, pair)
                each(piece, stage + 1, start, 1)
                each(piece, stage + 2, start, 0)
            elif step == 1:
                each(piece, stage, arrive, 1)
                each(piece, stage + 1, start, 1)
            else:
                arrive(dp_copies(piece, stage)[0][1]())
                place = (z % 2) * size
                for flag, source in ((1, came[stage - 1]), (0, pair)):

                    @pl.when(inner == flag)
                    def _():
                        if plan == NY:
                            summed(source, place, came[stage], 0, 2, mine[2])
                        else:
                            grads[piece][...] = summed(source, place, came[stage], 0, 1, None)

                if plan == NY:
                    each(piece, stage + 1, start)

    done = [(r.layer_out_v, r.layer_out), (r.feats_grad_v, r.feats_grad), (r.small_out_v, r.small_out)]
    done += list(zip(grads, grad_outs))

    def write_out(i):
        return pltpu.make_async_copy(*done[i], r.out_sem.at[i])

    def poll(point):
        for piece, stage in POLLS[point] if dp_bits else ():
            dp_finish(stage, piece)
            if stage == len(ARRIVING[PLANS[piece]]) - 1:
                write_out(3 + piece).start()

    pl.semaphore_wait(barrier, len(partners))
    load("ow").wait()
    ow_copy(1).start()
    ow_copy(0).start()
    for name in first:
        if name != "ow":
            load(name).wait()
    count = r.counts[0]
    gain_one, shift_one = row_of(r.gain_one), row_of(r.shift_one)
    q_bias = jnp.broadcast_to(row_of(r.q_bias), (128, cols)).T[:, :1]
    v_bias = jnp.broadcast_to(row_of(r.v_bias), (128, cols)).T[:, :1]
    lane = lax.broadcasted_iota(jnp.int32, (HD, BLOCK), 1)
    first_row = lax.broadcasted_iota(jnp.int32, (HD, BLOCK), 0) == 0
    one = jnp.where(first_row, 1.0, 0.0).astype(BF16)

    @pl.loop(0, blocks)
    def _(i):
        here = rows_at(i * BLOCK, BLOCK)
        load_feats(i).wait()
        std_rows, _ = standardized(r.feats[here, :].astype(F32))
        r.std_one[here, :] = std_rows.astype(BF16)
        normed = (std_rows * gain_one + shift_one).astype(BF16)
        r.normed[here, :] = normed
        projected = dot_nt(r.wqkv[...].reshape(3 * cols, width), normed)
        bias = jnp.where(jnp.logical_and(first_row, lane + i * BLOCK >= count), NEG, 0.0).astype(BF16)
        for h in range(heads):
            part = slice(h * HD, (h + 1) * HD)
            of_head = projected[3 * h * HD : 3 * (h + 1) * HD]
            query = ((of_head[:HD] + q_bias[part]).astype(BF16).astype(F32) * SCORE_SCALE).astype(BF16)
            keys = of_head[HD : 2 * HD].astype(BF16)
            values = (of_head[2 * HD :] + v_bias[part]).astype(BF16)
            r.query_t[i, h] = jnp.concatenate([query, one], axis=0)
            r.keys[h, here, :] = jnp.concatenate([keys, bias], axis=0).T
            r.values[h, here, :] = values.T
            r.keys_t[h, :, here] = keys
            r.values_t[h, :, here] = values

    @pl.loop(0, 2)
    def _(turn):
        units = [(block_of(2 * turn + place), h) for place in range(2) for h in range(heads)]
        scores = [dot(r.keys[h], r.query_t[block, h]) for block, h in units]
        for (block, h), score in zip(units, scores):
            peak = jnp.max(score, axis=0, keepdims=True)
            exped = jnp.exp(score - peak)
            total = jnp.sum(exped, axis=0, keepdims=True)
            exped = exped.astype(BF16)
            inverse = 1.0 / total
            r.exped[block, h] = exped
            r.inverse_total[block, h] = inverse
            mixed = dot(r.values_t[h], exped) * inverse
            r.mixed_t[block, pl.ds(pl.multiple_of(m * cols + h * HD, HD), HD), :] = mixed.astype(BF16)
        for place in range(2):
            mx_copy(1, turn, place).start()
            mx_copy(0, turn, place).start()

    for name in second:
        load(name).wait()
    slot = lax.broadcasted_iota(jnp.int32, (BLOCK, width), 0)
    r.key_acc[...] = jnp.zeros_like(r.key_acc)
    r.value_acc[...] = jnp.zeros_like(r.value_acc)

    @pl.loop(0, blocks)
    def _(i):
        here = rows_at(i * BLOCK, BLOCK)
        grad = r.og[here, :]
        grad = jnp.where(slot + i * BLOCK < count, grad.astype(F32), 0.0).astype(BF16)
        r.og[here, :] = grad
        r.hidden_grad[here, :] = dot_nt(grad, r.down[...])

    def mx_forward(turn):
        for place in range(2):
            mx_copy(1, turn, place).wait_recv()
            mx_copy(2, turn, place).start()

    def mx_arrive(kind, turn):
        for place in range(2):
            mx_copy(kind, turn, place).wait_recv()

    ow_copy(1).wait_recv()
    ow_copy(2).start()
    mx_forward(0)
    mx_arrive(0, 1)
    ow_copy(0).wait_recv()
    ow_copy(2).wait_recv()
    mx_arrive(2, 0)

    o_bias = row_of(r.o_bias)
    gain_two, shift_two = row_of(r.gain_two), row_of(r.shift_two)
    up_bias, down_bias = row_of(r.up_bias), row_of(r.down_bias)

    def feed_forward(pair, between):
        places = [rows_at(block_of(k) * BLOCK, BLOCK) for k in pair]
        attended = [dot_tn(r.mixed_t[block_of(k)], r.ow[...]) for k in pair]
        between()
        normed_two = []
        for k, here, value in zip(pair, places, attended):
            resid = r.feats[here, :].astype(F32) + (value + o_bias)
            std_rows, inverse = standardized(resid)
            if k == 0:
                r.resid[...] = resid
                r.std_two[...] = std_rows
                r.inverse_two[...] = inverse
            normed_two.append((std_rows * gain_two + shift_two).astype(BF16))
            r.normed_two[here, :] = normed_two[-1]
        pre_up = [dot(value, r.up[...]) + up_bias for value in normed_two]
        pre_grads = []
        for here, value in zip(places, pre_up):
            hidden, slope = gelu_pair(value)
            r.hidden[here, :] = hidden.astype(BF16)
            pre_grads.append((r.hidden_grad[here, :] * slope).astype(BF16))
            r.pre_grad[here, :] = pre_grads[-1]
        return pre_grads

    def feed_forward_out(k):
        return dot(r.hidden[rows_at(block_of(k) * BLOCK, BLOCK), :], r.down[...])

    pre_grads = feed_forward((3, 2), lambda: None)
    r.bk_tx[0] = dot_nt(pre_grads[0], r.up[...]).astype(BF16)
    rs_copy(BK, 0).start()
    mx_forward(1)
    r.back[...] = dot_nt(pre_grads[1], r.up[...])

    def send_back():
        rs_copy(BK, 0).wait_recv()
        r.bk_tx[1] = (r.back[...] + r.bk_rx[0].astype(F32)).astype(BF16)
        rs_copy(BK, 1).start()

    mx_arrive(0, 0)
    mx_arrive(2, 1)
    pre_grads = feed_forward((1, 0), send_back)

    def grad_tiles(left, right, pieces):
        right_all = right[...]

        @pl.loop(0, 2)
        def _(t):
            value = dot_tn(left[:, rows_at(t * 384, 384)], right_all)
            store_piece(pieces[0], t, value[:, :384])
            store_piece(pieces[1], t, value[:, 384:])

        dp_start(*pieces)

    grad_tiles(r.og, r.hidden, (DOWN0, DOWN1))
    grad_tiles(r.normed_two, r.pre_grad, (UP0, UP1))

    r.ml_tx[0] = feed_forward_out(3).astype(BF16)
    rs_copy(ML, 0).start()
    ml_x = feed_forward_out(2)
    r.bk_tx[2] = dot_nt(r.pre_grad[rows_at(block_of(1) * BLOCK, BLOCK), :], r.up[...]).astype(BF16)
    rs_copy(BK, 2).start()
    rs_copy(ML, 0).wait_recv()
    r.ml_tx[1] = (ml_x + r.ml_rx[0].astype(F32)).astype(BF16)
    r.back[...] = dot_nt(r.pre_grad[own, :], r.up[...])
    r.ml_tx[2] = feed_forward_out(1).astype(BF16)
    rs_copy(ML, 2).start()
    r.ml_own[...] = feed_forward_out(0)
    ones = jnp.ones((8, rows), BF16)
    r.small[6:7, :] = dot(ones, r.pre_grad[...])[:1]

    rs_copy(BK, 2).wait_recv()
    rs_copy(BK, 1).wait_recv()
    back = r.back[...] + r.bk_rx[2].astype(F32) + r.bk_rx[1].astype(F32)
    std_rows, inverse = r.std_two[...], r.inverse_two[...]
    own_grad = r.og[own, :].astype(F32)
    resid_grad = own_grad + norm_back(std_rows, inverse, gain_two, back)
    resid_low = resid_grad.astype(BF16)
    for k in (2, 3, 1):
        target_heads = r.ow[pl.ds(pl.multiple_of(mp_peers[k] * cols, 64), cols), :]
        r.mg_tx[k - 1] = dot_nt(target_heads, resid_low).astype(BF16)
        mg_copy(k).start()
    r.mixed_grad_t[m] = dot_nt(r.ow[own_heads, :], resid_low).astype(BF16)
    r.resid_grad[...] = resid_grad
    r.resid_low[c] = resid_low
    rl_copy().start()
    r.back[...] = back

    def attend_back(block):
        for h in range(heads):
            part = slice(h * HD, (h + 1) * HD)
            exped = r.exped[block, h]
            scaled = (r.mixed_grad_t[block, part, :].astype(F32) * r.inverse_total[block, h]).astype(BF16)
            mixed = r.mixed_t[block, pl.ds(pl.multiple_of(m * cols + h * HD, HD), HD), :]
            inner_product = column_sum(scaled.astype(F32) * mixed.astype(F32))
            prob_grad = dot(r.values[h], scaled)
            score_grad = (exped.astype(F32) * (prob_grad - inner_product)).astype(BF16)
            r.value_acc[h] += dot_nt(scaled, exped)
            r.key_acc[h] += dot_nt(r.query_t[block, h][:HD], score_grad)
            query_grad = dot(r.keys_t[h], score_grad) * SCORE_SCALE
            r.dqkv_t[3 * h * HD : (3 * h + 1) * HD, rows_at(block * BLOCK, BLOCK)] = query_grad.astype(BF16)

    def out_partial(head_rows):
        value = dot(r.mixed_t[m, head_rows, :], r.resid_low[c])
        return value + dot(r.mixed_t[cp, head_rows, :], r.resid_low[1 - c])

    @pl.loop(0, blocks)
    def _(i):
        @pl.when(i == 1)
        def _():
            poll(0)
            mg_copy(1).wait_recv()
            rl_copy().wait_recv()
            r.go_tx[...] = out_partial(pl.ds(pl.multiple_of(xp * cols, 64), cols)).astype(BF16)
            go_copy().start()
            rs_copy(ML, 1).start()

        @pl.when(i == 2)
        def _():
            poll(1)
            mg_copy(2).wait_recv()

        @pl.when(i == 3)
        def _():
            poll(2)
            mg_copy(3).wait_recv()

        attend_back(block_of(i))

    poll(3)

    for h in range(heads):
        row = 3 * h * HD
        r.dqkv_t[row + HD : row + 2 * HD, :] = r.key_acc[h].astype(BF16)
        r.dqkv_t[row + 2 * HD : row + 3 * HD, :] = r.value_acc[h].astype(BF16)
    value = dot(r.dqkv_t[...], r.normed[...])
    if dp_bits:
        value = value.astype(BF16)
    for t in range(2):
        for h in range(heads):
            store_piece(HEAD0 + h, t, value[h * cols : (h + 1) * cols, t * 384 : (t + 1) * 384].T)
    dp_start(HEAD0, HEAD1, HEAD2)
    poll(4)

    for step in range(3):
        rs_copy(BK, step).wait_send()
    r.gain_sum[...] = jnp.zeros_like(r.gain_sum)
    r.shift_sum[...] = jnp.zeros_like(r.shift_sum)

    def input_block(i):
        here = rows_at(block_of(3 - i) * BLOCK, BLOCK)
        part = dot_tn(r.dqkv_t[:, here], r.wqkv[...].reshape(3 * cols, width))

        @pl.when(i == 0)
        def _():
            r.bk_tx[0] = part.astype(BF16)
            rs_copy(IN, 0).start()

        @pl.when(i == 1)
        def _():
            rs_copy(IN, 0).wait_recv()
            r.bk_tx[1] = (part + r.in_rx[0].astype(F32)).astype(BF16)
            rs_copy(IN, 1).start()

        @pl.when(i == 2)
        def _():
            r.bk_tx[2] = part.astype(BF16)
            rs_copy(IN, 2).start()

        @pl.when(i == 3)
        def _():
            r.back[...] = part

        r.gain_sum[...] += column_sum(part * r.std_one[here, :].astype(F32))
        r.shift_sum[...] += column_sum(part)

    input_block(0)
    partial = out_partial(own_heads)
    input_block(1)
    poll(5)

    go_copy().wait_recv()
    value = partial + r.go_rx[...].astype(F32)
    for t in range(2):
        store_piece(OUT, t, value[:, t * 384 : (t + 1) * 384].T)
    dp_start(OUT)
    poll(6)

    r.small[2:3, :] = column_sum(r.resid_low[c].astype(F32))
    r.small[3:4, :] = column_sum(r.back[...] * r.std_two[...])
    r.small[4:5, :] = column_sum(r.back[...])
    r.small[5:6, :] = column_sum(r.og[own, :].astype(F32))

    @pl.loop(0, 2)
    def _(i):
        input_block(i + 2)

    poll(7)

    r.small[0:1, :] = r.gain_sum[...]
    r.small[1:2, :] = r.shift_sum[...]
    bias_sums = dot_nt(jnp.ones((8, rows), BF16), r.dqkv_t[...])[:1]
    q_sums = jnp.concatenate([bias_sums[:, 3 * h * HD : (3 * h + 1) * HD] for h in range(heads)], axis=1)
    v_sums = jnp.concatenate([bias_sums[:, (3 * h + 2) * HD : 3 * (h + 1) * HD] for h in range(heads)], axis=1)
    if dp_bits:
        dp_size = 1 << dp_bits
        share, head_share = width // dp_size, cols // dp_size
        blank = jnp.zeros((1, 128 - 2 * head_share), F32)
        for peer in range(dp_size):
            r.small_tx[peer, 0:7, :share] = r.small[0:7, peer * share : (peer + 1) * share]
            of_peer = slice(peer * head_share, (peer + 1) * head_share)
            r.small_tx[peer, 7:8, :] = jnp.concatenate([q_sums[:, of_peer], v_sums[:, of_peer], blank], axis=1)
        for k in range(1, dp_size):
            sd_copy(k).start()
    else:
        r.small[7:8, :] = jnp.concatenate([q_sums, v_sums, jnp.zeros((1, width - 2 * cols), F32)], axis=1)

    poll(8)
    rs_copy(ML, 1).wait_recv()
    rs_copy(ML, 2).wait_recv()
    mlp = r.ml_own[...] + r.ml_rx[2].astype(F32) + r.ml_rx[1].astype(F32)
    r.layer_out_v[...] = (r.resid[...] + (mlp + down_bias)).astype(BF16)
    write_out(0).start()
    std_rows, inverse = standardized(r.feats[own, :].astype(F32))
    poll(9)

    if dp_bits:
        total = r.small_tx[lax.axis_index(DP)]
        for k in range(1, 1 << dp_bits):
            sd_copy(k).wait_recv()
            total = total + r.sd_rx[k - 1]
        r.small_dp[...] = total
    else:
        r.small_dp[...] = r.small[...]
    for k in mp_peers:
        sg_copy(k).start()

    poll(10)
    rs_copy(IN, 2).wait_recv()
    rs_copy(IN, 1).wait_recv()
    back = r.back[...] + r.in_rx[2].astype(F32) + r.in_rx[1].astype(F32)
    r.feats_grad_v[...] = (r.resid_grad[...] + norm_back(std_rows, inverse, gain_one, back)).astype(BF16)
    write_out(1).start()

    total = r.small_dp[...]
    for k in mp_peers:
        sg_copy(k).wait_recv()
        of_peer = r.sg_rx[k - 1]
        total = total + jnp.where(lax.broadcasted_iota(jnp.int32, of_peer.shape, 0) < 6, of_peer, 0.0)
    r.small_out_v[...] = total
    write_out(2).start()
    poll(11)
    if not dp_bits:
        for piece in range(len(PLANS)):
            write_out(3 + piece).start()

    for i in range(len(done)):
        write_out(i).wait()
    for kind in range(3):
        ow_copy(kind).wait_send()
        rs_copy(IN, kind).wait_send()
        rs_copy(ML, kind).wait_send()
        for turn in range(2):
            for place in range(2):
                mx_copy(kind, turn, place).wait_send()
    rl_copy().wait_send()
    go_copy().wait_send()
    for k in mp_peers:
        mg_copy(k).wait_send()
        sg_copy(k).wait_send()
    if dp_bits:
        for k in range(1, 1 << dp_bits):
            sd_copy(k).wait_send()
        for piece, plan in enumerate(PLANS):
            for stage in range(len(ARRIVING[plan])):
                each(piece, stage, leave)


def finish_kernel(names, *refs):
    r = types.SimpleNamespace(**dict(zip(names, refs)))
    grads = refs[len(names) :]
    shard = r.up.shape[0]
    unpacked = (r.head0, r.head1, r.head2, r.o)
    incoming = [
        (r.small_out, r.small), (r.layer_out, r.layer), (r.feats_grad, r.feats), *zip(grads[HEAD0:], unpacked),
        (grads[UP0], r.up.at[:, pl.ds(0, 384)]), (grads[UP1], r.up.at[:, pl.ds(384, 384)]),
        (grads[DOWN0], r.down.at[:, pl.ds(0, 384)]), (grads[DOWN1], r.down.at[:, pl.ds(384, 384)]),
    ]
    outgoing = [
        (r.layer, r.out_layer), (r.feats, r.out_feats), (r.up, r.out_up), (r.down, r.out_down), (r.q, r.out_q),
        (r.k, r.out_k), (r.v, r.out_v), (r.o_t, r.out_o), (r.up_bias, r.out_up_bias),
    ]
    vectors = (r.out_gain_one, r.out_shift_one, r.out_o_bias, r.out_gain_two, r.out_shift_two, r.out_down_bias, r.out_q_bias,
               r.out_v_bias)
    outgoing += [(r.pieces.at[i], target) for i, target in enumerate(vectors)]

    def take(i):
        return pltpu.make_async_copy(*incoming[i], r.in_sem.at[i])

    def give(i):
        return pltpu.make_async_copy(*outgoing[i], r.out_sem.at[i])

    for i in range(len(incoming)):
        take(i).start()
    take(0).wait()
    m = lax.axis_index(MP)
    small = r.small[...]
    piece = r.out_gain_one.shape[0]
    mine = pltpu.roll(small, (128 - m * piece) % 128, 1)
    for i in range(6):
        r.pieces[i] = mine[i, :piece]
    r.pieces[6] = small[7, :piece]
    r.pieces[7] = small[7, piece : 2 * piece]
    r.up_bias[...] = small[6, :shard]
    for i in range(8, len(outgoing)):
        give(i).start()
    for i in (1, 2):
        take(i).wait()
        give(i - 1).start()
    for i in range(3, 7):
        take(i).wait()
    heads = [jnp.concatenate([ref[:, :192], ref[:, 192:]], axis=0) for ref in unpacked]
    for i, target in enumerate((r.q, r.k, r.v)):
        target[...] = jnp.concatenate([value[:, i * HD : (i + 1) * HD] for value in heads[:3]], axis=1)
        give(4 + i).start()
    r.o_t[...] = heads[3].T
    give(7).start()
    for i in range(7, 11):
        take(i).wait()
        if i % 2 == 0:
            give((i - 4) // 2).start()
    for i in range(len(outgoing)):
        give(i).wait()


def layer_call(dp_size, clip_feats, counts, gain_one, shift_one, q_weight, k_weight, v_weight, q_bias, v_bias, o_weight,
               o_bias, gain_two, shift_two, up_weight, up_bias, down_weight, down_bias, out_grad):
    rows, width = clip_feats.shape
    cols = q_weight.shape[1]
    heads = cols // HD
    hidden_cols = up_weight.shape[1]
    dp_bits = 3 if dp_size == 8 else 0
    vmem = pl.BlockSpec(memory_space=pltpu.VMEM)
    anywhere = pl.BlockSpec(memory_space=pl.ANY)
    by_head = (heads, HD, width)
    inputs = dict(
        gain_one_hbm=(gain_one, anywhere), shift_one_hbm=(shift_one, anywhere), q_bias_hbm=(q_bias, anywhere),
        v_bias_hbm=(v_bias, anywhere), o_bias_hbm=(o_bias, anywhere), gain_two_hbm=(gain_two, anywhere),
        shift_two_hbm=(shift_two, anywhere), up_bias_hbm=(up_bias, anywhere),
        down_bias_hbm=(down_bias, anywhere), counts_hbm=(counts, anywhere),
        feats_hbm=(clip_feats, anywhere), qw_hbm=(q_weight.T.reshape(by_head), anywhere),
        kw_hbm=(k_weight.T.reshape(by_head), anywhere), vw_hbm=(v_weight.T.reshape(by_head), anywhere),
        ow_hbm=(o_weight, anywhere), up_hbm=(up_weight, anywhere),
        down_hbm=(down_weight, anywhere), og_hbm=(out_grad, anywhere),
    )
    shard = width // dp_size if dp_bits else width
    small_shape = (8, 128) if dp_bits else (8, width)
    outputs = dict(layer_out=((BLOCK, width), BF16), feats_grad=((BLOCK, width), BF16), small_out=(small_shape, F32))
    grads = [(packed_shape(i, shard) if dp_bits else (width, COLUMNS[i]), F32) for i in range(len(PLANS))]
    piece = (BLOCK, width)
    scratch = dict(
        gain_one=((width,), BF16), shift_one=((width,), BF16), q_bias=((cols,), BF16), v_bias=((cols,), BF16),
        o_bias=((width,), BF16), gain_two=((width,), BF16), shift_two=((width,), BF16),
        up_bias=((hidden_cols,), BF16), down_bias=((width,), BF16),
        feats=((rows, width), BF16), wqkv=((heads, 3 * HD, width), BF16), ow=((width, width), BF16),
        og=((rows, width), BF16), down=((hidden_cols, width), BF16), up=((width, hidden_cols), BF16),
        normed=((rows, width), BF16), std_one=((rows, width), BF16),
        query_t=((rows // BLOCK, heads, 2 * HD, BLOCK), BF16), keys=((heads, rows, 2 * HD), BF16), values=((heads, rows, HD), BF16),
        keys_t=((heads, HD, rows), BF16), values_t=((heads, HD, rows), BF16), mixed_t=((rows // BLOCK, width, BLOCK), BF16),
        exped=((rows // BLOCK, heads, rows, BLOCK), BF16), inverse_total=((rows // BLOCK, heads, 1, BLOCK), F32), hidden_grad=((rows, hidden_cols), F32), resid=(piece, F32),
        normed_two=((rows, width), BF16), hidden=((rows, hidden_cols), BF16), pre_grad=((rows, hidden_cols), BF16),
        back=(piece, F32), resid_grad=(piece, F32),
        resid_low=((2,) + piece, BF16), go_tx=((cols, width), BF16), go_rx=((cols, width), BF16), std_two=(piece, F32), inverse_two=((BLOCK, 1), F32), ml_own=(piece, F32),
        bk_tx=((3,) + piece, BF16), bk_rx=((3,) + piece, BF16), ml_tx=((3,) + piece, BF16),
        ml_rx=((3,) + piece, BF16), in_rx=((3,) + piece, BF16),
        mg_tx=((3, cols, BLOCK), BF16), mixed_grad_t=((rows // BLOCK, cols, BLOCK), BF16),
        key_acc=((heads, HD, rows), F32), value_acc=((heads, HD, rows), F32), dqkv_t=((3 * cols, rows), BF16),
        gain_sum=((1, width), F32), shift_sum=((1, width), F32),
        small=((8, width), F32), small_dp=(small_shape, F32), sg_rx=((3,) + small_shape, F32),
    )
    scratch.update({name + "_v": spec for name, spec in outputs.items()})
    of_pieces = list(grads)
    if dp_bits:
        scratch.update(
            small_tx=((dp_size,) + small_shape, F32), sd_rx=((dp_size - 1,) + small_shape, F32)
        )
        for table in (HELD, ARRIVING):
            for i, plan in enumerate(PLANS):
                of_pieces += [((count,) + packed_shape(i, shard), BF16) for count in table[plan]]
    copies = 29 + 12 + 4 * len(PLANS)
    scalars = dict(
        counts=pltpu.SMEM((1,), jnp.int32), load_sem=pltpu.SemaphoreType.DMA((17 + rows // BLOCK,)),
        out_sem=pltpu.SemaphoreType.DMA((len(outputs) + len(grads),)), send_sem=pltpu.SemaphoreType.DMA((copies,)),
        recv_sem=pltpu.SemaphoreType.DMA((copies,)),
    )
    names = list(inputs) + list(outputs)
    kernel_names = [*inputs, *outputs, *scratch, *scalars]

    def kernel(*refs):
        refs = list(refs)
        grad_refs = refs[len(names) : len(names) + len(grads)]
        rest = refs[len(names) + len(grads) :]
        named = len(scratch) + len(scalars)
        layer_kernel(kernel_names, dp_bits, *refs[: len(names)], *rest[:named], *grad_refs, *rest[named:])

    results = pl.pallas_call(
        kernel,
        out_shape=[jax.ShapeDtypeStruct(*spec) for spec in [*outputs.values(), *grads]],
        in_specs=[spec for _, spec in inputs.values()],
        out_specs=[anywhere] * (len(outputs) + len(grads)),
        scratch_shapes=[pltpu.VMEM(*spec) for spec in scratch.values()] + list(scalars.values())
        + [pltpu.VMEM(*spec) for spec in of_pieces],
        compiler_params=pltpu.CompilerParams(collective_id=0, has_side_effects=True, vmem_limit_bytes=67043328),
        name="layer",
    )(*[value for value, _ in inputs.values()])
    return dict(zip(outputs, results)), results[len(outputs) :]


def finish_call(out, grads, cols, hidden_cols):
    shard, width = COLUMNS[UP0] // 4, out["layer_out"].shape[1]
    rows = ((BLOCK, width), BF16)
    small = ((shard // 4,), F32)
    head = ((shard, cols), F32)
    shapes = dict(
        out_layer=rows, out_feats=rows, out_gain_one=small, out_shift_one=small, out_q=head, out_k=head, out_v=head,
        out_q_bias=small, out_v_bias=small, out_o=((cols, shard), F32), out_o_bias=small, out_gain_two=small,
        out_shift_two=small, out_up=((shard, hidden_cols), F32), out_up_bias=((shard,), F32),
        out_down=((shard, hidden_cols), F32), out_down_bias=small,
    )
    packed = (packed_shape(OUT, shard), F32)
    scratch = dict(
        small=((8, 128), F32), layer=rows, feats=rows, head0=packed, head1=packed, head2=packed, o=packed,
        up=((shard, hidden_cols), F32), down=((shard, hidden_cols), F32), q=head, k=head, v=head, o_t=((cols, shard), F32),
        up_bias=((shard,), F32), pieces=((8, shard // 4), F32),
    )
    sems = dict(in_sem=pltpu.SemaphoreType.DMA((11,)), out_sem=pltpu.SemaphoreType.DMA((17,)))
    names = [*out, *shapes, *scratch, *sems]

    def kernel(*refs):
        count = len(out) + len(grads)
        finish_kernel(names, *refs[: len(out)], *refs[count:], *refs[len(out) : count])

    anywhere = pl.BlockSpec(memory_space=pl.ANY)
    results = pl.pallas_call(
        kernel,
        out_shape=[jax.ShapeDtypeStruct(*spec) for spec in shapes.values()],
        in_specs=[anywhere] * (len(out) + len(grads)),
        out_specs=[anywhere] * len(shapes),
        scratch_shapes=[pltpu.VMEM(*spec) for spec in scratch.values()] + list(sems.values()),
        name="finish",
    )(*out.values(), *grads)
    return (*results[:15], results[15].T, results[16])


def shards(dp_size, *args):
    out, grads = layer_call(dp_size, *args)
    cols, hidden_cols = args[4].shape[1], args[13].shape[1]
    if dp_size == 8:
        return finish_call(out, grads, cols, hidden_cols)

    def over(value, dim):
        return lax.psum_scatter(value, DP, scatter_dimension=dim, tiled=True)

    small = lax.psum(out["small_out"], DP)
    width = small.shape[1]
    d, m = lax.axis_index(DP), lax.axis_index(MP)
    piece = width // (dp_size * 4)
    group = [lax.dynamic_slice(small, (i, (d * 4 + m) * piece), (1, piece)).reshape(piece) for i in range(6)]
    up_piece = hidden_cols // dp_size
    head_piece = cols // dp_size
    up_bias = lax.dynamic_slice(small, (6, d * up_piece), (1, up_piece)).reshape(up_piece)
    q_bias = lax.dynamic_slice(small, (7, d * head_piece), (1, head_piece)).reshape(head_piece)
    v_bias = lax.dynamic_slice(small, (7, cols + d * head_piece), (1, head_piece)).reshape(head_piece)
    heads = grads[HEAD0 : HEAD2 + 1]
    q_grad, k_grad, v_grad = (
        jnp.concatenate([value[:, i * HD : (i + 1) * HD] for value in heads], axis=1) for i in range(3)
    )
    up_grad = jnp.concatenate([grads[UP0], grads[UP1]], axis=1)
    down_grad = jnp.concatenate([grads[DOWN0], grads[DOWN1]], axis=1)
    return (
        out["layer_out"], out["feats_grad"], group[0], group[1], over(q_grad, 0), over(k_grad, 0), over(v_grad, 0),
        q_bias, v_bias, over(grads[OUT].T, 1), group[2], group[3], group[4], over(up_grad, 0), up_bias,
        over(down_grad.T, 1), group[5],
    )


def solution(mesh):
    placed = (
        P(DP, None), P(DP), P(), P(), P(None, MP), P(None, MP), P(None, MP), P(MP), P(MP), P(MP, None),
        P(), P(), P(), P(None, MP), P(MP), P(MP, None), P(), P(DP, None),
    )
    return jax.shard_map(
        functools.partial(shards, mesh.shape[DP]),
        mesh=mesh,
        in_specs=placed,
        out_specs=(
            P((DP, MP), None), P((DP, MP), None), P((DP, MP)), P((DP, MP)), P(DP, MP), P(DP, MP),
            P(DP, MP), P((MP, DP)), P((MP, DP)), P(MP, DP), P((DP, MP)), P((DP, MP)),
            P((DP, MP)), P(DP, MP), P((MP, DP)), P(MP, DP), P((DP, MP)),
        ),
        check_vma=False,
    )
```

```python
import functools
import types

import jax
import jax.numpy as jnp
from jax import lax
from jax.experimental import pallas as pl
from jax.experimental.pallas import tpu as pltpu
from jax.sharding import PartitionSpec as P

HD = 64
NORM_EPSILON = 1e-06
SCORE_SCALE = 0.125
BLOCK = 256
MESH = pl.DeviceIdType.MESH
F32 = jnp.float32
BF16 = jnp.bfloat16
DP, MP = "dp", "mp"
INV_SQRT2 = 0.7071067811865476
INV_SQRT_2PI = 0.3989422804014327
NEG = -1e30

YN, NY, YD, ZYZ, YZZ = range(5)
HALVED = {ZYZ: (1, 0, 2), YZZ: (0, 1, 2)}
DOWN0, DOWN1, UP0, UP1, HEAD0, HEAD1, HEAD2, OUT = range(8)
PLANS = (YZZ, NY, YN, YZZ, YZZ, YZZ, YZZ, YZZ)
COLUMNS = (384, 384, 384, 384, 192, 192, 192, 192)
HELD = {YN: (8, 4, 2), NY: (8, 4, 2), YD: (8, 4), ZYZ: (8, 4, 2), YZZ: (8, 4, 2)}
ARRIVING = {YN: (4, 2, 2, 1), NY: (4, 4, 2, 1), YD: (4, 3), ZYZ: (4, 2, 1), YZZ: (4, 2, 1)}


POLLS = (
    ((DOWN0, 0), (DOWN1, 0)),
    (),
    ((UP0, 0),),
    ((DOWN0, 1),),
    ((DOWN1, 1),),
    ((UP1, 0),),
    ((UP0, 1),),
    (),
    ((HEAD0, 0), (DOWN1, 2), (UP1, 1), (DOWN0, 2)),
    ((HEAD1, 0), (UP0, 2), (HEAD0, 1), (HEAD2, 0)),
    ((HEAD1, 1), (OUT, 0), (UP0, 3), (DOWN1, 3), (HEAD2, 1), (UP1, 2), (OUT, 1)),
    ((HEAD0, 2), (HEAD1, 2), (HEAD2, 2), (OUT, 2)),
)


def packed_shape(piece, rows):
    columns = COLUMNS[piece]
    return (rows, columns) if columns == 384 else (rows // 2, 2 * columns)


def dot(left, right):
    return jnp.dot(left, right, preferred_element_type=F32)


def dot_nt(left, right):
    return lax.dot_general(left, right, (((1,), (1,)), ((), ())), preferred_element_type=F32)


def dot_tn(left, right):
    return lax.dot_general(left, right, (((0,), (0,)), ((), ())), preferred_element_type=F32)


def standardized(values):
    centered = values - jnp.mean(values, axis=-1, keepdims=True)
    variance = jnp.mean(centered * centered, axis=-1, keepdims=True)
    inverse = lax.rsqrt(variance + NORM_EPSILON)
    return centered * inverse, inverse


def norm_back(std_rows, inverse, gain, grad):
    scaled = gain * grad
    mean_scaled = jnp.mean(scaled, axis=-1, keepdims=True)
    mean_inner = jnp.mean(scaled * std_rows, axis=-1, keepdims=True)
    return inverse * (scaled - mean_scaled - std_rows * mean_inner)


def gelu_pair(values):
    bell = jnp.exp(-0.5 * (values * values))
    t = 1.0 / (1.0 + (0.3275911 * INV_SQRT2) * jnp.abs(values))
    tail = t * (0.127414796 + t * (-0.142248368 + t * (0.7107068705 + t * (-0.7265760135 + t * 0.5307027145)))) * bell
    phi = jnp.where(values >= 0.0, 1.0 - tail, tail)
    return values * phi, phi + values * (bell * INV_SQRT_2PI)


def column_sum(values):
    return jnp.sum(values, axis=0, keepdims=True)


def row_of(ref):
    return ref[...].astype(F32).reshape(1, -1)


def layer_kernel(names, dp_bits, *refs):
    r = types.SimpleNamespace(**dict(zip(names, refs)))
    of_pieces = iter(refs[len(names) :])
    grad_outs = [next(of_pieces) for _ in PLANS]
    grads = [next(of_pieces) for _ in PLANS]
    held = [[next(of_pieces) for _ in HELD[plan]] for plan in PLANS] if dp_bits else []
    arrived = [[next(of_pieces) for _ in ARRIVING[plan]] for plan in PLANS] if dp_bits else []
    rows, width = r.feats_hbm.shape
    heads = r.qw_hbm.shape[0]
    cols = heads * HD
    blocks = rows // BLOCK

    m = lax.axis_index(MP)
    c = m % 2
    x = m // 2
    cp = m + 1 - 2 * c
    xp = m + 2 - 4 * x

    def bit_of(bit):
        return (lax.axis_index(DP) // (1 << bit)) % 2

    def dp_peer(mask):
        peer = lax.axis_index(DP)
        for bit in range(3):
            if mask >> bit & 1:
                peer = peer + (1 << bit) * (1 - 2 * bit_of(bit))
        return peer

    def block_of(k):
        kx, kc = k // 2, k % 2
        return 2 * (x + kx - 2 * x * kx) + (c + kc - 2 * c * kc)

    def rows_at(start, size):
        return pl.ds(pl.multiple_of(start, size), size)

    own_heads = pl.ds(pl.multiple_of(m * cols, 64), cols)
    own = rows_at(m * BLOCK, BLOCK)

    first = dict(
        counts=(r.counts_hbm, r.counts), ow=(r.ow_hbm, r.ow.at[own_heads, :]), qw=(r.qw_hbm, r.wqkv.at[:, pl.ds(0, HD), :]),
        kw=(r.kw_hbm, r.wqkv.at[:, pl.ds(HD, HD), :]), vw=(r.vw_hbm, r.wqkv.at[:, pl.ds(2 * HD, HD), :]),
        gain_one=(r.gain_one_hbm, r.gain_one), shift_one=(r.shift_one_hbm, r.shift_one), q_bias=(r.q_bias_hbm, r.q_bias),
        v_bias=(r.v_bias_hbm, r.v_bias),
    )
    second = dict(
        o_bias=(r.o_bias_hbm, r.o_bias), gain_two=(r.gain_two_hbm, r.gain_two), shift_two=(r.shift_two_hbm, r.shift_two),
        up_bias=(r.up_bias_hbm, r.up_bias), down_bias=(r.down_bias_hbm, r.down_bias), og=(r.og_hbm, r.og),
        down=(r.down_hbm, r.down), up=(r.up_hbm, r.up),
    )
    loads = {**first, **second}
    load_index = {name: i for i, name in enumerate(loads)}

    def load(name):
        return pltpu.make_async_copy(*loads[name], r.load_sem.at[load_index[name]])

    def load_feats(i):
        here = rows_at(i * BLOCK, BLOCK)
        return pltpu.make_async_copy(r.feats_hbm.at[here, :], r.feats.at[here, :], r.load_sem.at[len(loads) + i])

    for name in first:
        load(name).start()
    for i in range(blocks):
        load_feats(i).start()
    for name in second:
        load(name).start()

    barrier = pltpu.get_barrier_semaphore()
    mp_peers = {1: cp, 2: xp, 3: block_of(3)}
    partners = [{MP: peer} for peer in mp_peers.values()] + [{DP: dp_peer(k)} for k in range(1, 1 << dp_bits)]
    for partner in partners:
        pl.semaphore_signal(barrier, inc=1, device_id=partner, device_id_type=MESH)

    def remote(index, source, target, partner):
        return pltpu.make_async_remote_copy(
            src_ref=source, dst_ref=target, send_sem=r.send_sem.at[index], recv_sem=r.recv_sem.at[index],
            device_id=partner, device_id_type=MESH,
        )

    OW, RL, BK, ML, IN, MG, SG, SD, MX = 0, 3, 6, 9, 13, 16, 19, 22, 29
    PIECE = MX + 12

    def ow_copy(kind):
        view = r.ow.at[pl.ds(pl.multiple_of((m, m, xp)[kind] * cols, 64), cols), :]
        return remote(OW + kind, view, view, {MP: (cp, xp, cp)[kind]})

    def mx_copy(kind, turn, place):
        owner = (m, m, xp)[kind]
        block = block_of(2 * turn + place if kind < 2 else 2 * (1 - turn) + place)
        view = r.mixed_t.at[block, pl.ds(pl.multiple_of(owner * cols, 64), cols), :]
        return remote(MX + (kind * 2 + turn) * 2 + place, view, view, {MP: (cp, xp, cp)[kind]})

    def rl_copy():
        return remote(RL, r.resid_low.at[c], r.resid_low.at[c], {MP: cp})

    def go_copy():
        return remote(RL + 1, r.go_tx, r.go_rx, {MP: xp})

    def rs_copy(base, step):
        send, receive = {BK: (r.bk_tx, r.bk_rx), ML: (r.ml_tx, r.ml_rx), IN: (r.bk_tx, r.in_rx)}[base]
        return remote(base + step, send.at[step], receive.at[step], {MP: (cp, xp, cp)[step]})

    def mg_copy(k):
        return remote(MG + k - 1, r.mg_tx.at[k - 1], r.mixed_grad_t.at[m], {MP: mp_peers[k]})

    def sg_copy(k):
        return remote(SG + k - 1, r.small_dp, r.sg_rx.at[k - 1], {MP: mp_peers[k]})

    def sd_copy(k):
        return remote(SD + k - 1, r.small_tx.at[dp_peer(k)], r.sd_rx.at[k - 1], {DP: dp_peer(k)})

    def store_piece(piece, tile, value):
        if not dp_bits:
            grads[piece][pl.ds(tile * 384, 384), :] = value
            return
        columns = COLUMNS[piece]
        weight = {YN: (4, 1, 2), YD: (4, 1, 2), NY: (1, 2, 4), ZYZ: (2, 4, 1), YZZ: (4, 2, 1)}[PLANS[piece]]
        for j in range(4):
            place = (j % 2) * weight[0] + (j // 2) * weight[1] + tile * weight[2]
            block = value[j * 96 : (j + 1) * 96].astype(BF16)
            if columns == 384:
                held[piece][0][place] = block
            else:
                held[piece][0][place, :, :columns] = block[:48]
                held[piece][0][place, :, columns:] = block[48:]

    y, z = bit_of(0), lax.axis_index(DP) // 2
    side, inner = z // 2, ((z + 1) // 2) % 2
    facing = side + inner - 2 * side * inner

    def part(ref, start, count):
        return ref.at[pl.ds(start, count)]

    def dp_remote(piece, stage, source, mask, target=None):
        target = arrived[piece][stage] if target is None else target
        return remote(PIECE + 4 * piece + stage, source, target, {DP: dp_peer(mask)})

    def dp_copies(piece, stage):
        plan, mine = PLANS[piece], held[piece]
        if plan in HALVED:
            bit = HALVED[plan][stage]
            count = 4 >> stage
            return [(None, lambda: dp_remote(piece, stage, part(mine[stage], (1 - bit_of(bit)) * count, count), 1 << bit))]
        if plan == YD and stage == 1:
            return [
                (None, lambda k=k: remote(PIECE + 4 * piece + k, mine[1].at[dp_peer(2 * k) // 2], arrived[piece][1].at[k - 1],
                                          {DP: dp_peer(2 * k)}))
                for k in (3, 2, 1)
            ]
        if stage == (3 if plan == NY else 0):
            count = 1 if plan == NY else 4
            source = mine[2] if plan == NY else mine[0]
            return [(None, lambda: dp_remote(piece, stage, part(source, (1 - y) * count, count), 1))]
        size = 2 if plan == NY else 1
        step = stage if plan == NY else stage - 1
        pair = mine[1 if plan == NY else 2]
        if step == 0:
            return [(None, lambda: dp_remote(piece, stage, part(mine[0 if plan == NY else 1], 2 * size * (1 - facing), 2 * size), 2))]
        if step == 1:
            return [(1, lambda: dp_remote(piece, stage, pair, 6))]
        place = (1 - z % 2) * size
        return [
            (1, lambda: dp_remote(piece, stage, part(arrived[piece][stage - 1], place, size), 2)),
            (0, lambda: dp_remote(piece, stage, part(pair, place, size), 2)),
        ]

    def each(piece, stage, action, only=None):
        for flag, make in dp_copies(piece, stage):
            if flag is None:
                action(make())
            elif only is None or only == flag:

                @pl.when(inner == flag)
                def _():
                    action(make())

    def start(copy):
        copy.start()

    def arrive(copy):
        copy.wait_recv()

    def leave(copy):
        copy.wait_send()

    def dp_start(*pieces):
        if dp_bits:
            for piece in pieces:
                each(piece, 0, start)

    def summed(first_ref, first_place, second_ref, second_place, count, target):
        for i in range(count):
            total = first_ref[first_place + i].astype(F32) + second_ref[second_place + i].astype(F32)
            if target is None:
                return total
            target[i] = total.astype(BF16)

    def dp_finish(stage, *pieces):
        for piece in pieces if dp_bits else ():
            plan, mine, came = PLANS[piece], held[piece], arrived[piece]
            if plan in HALVED:
                each(piece, stage, arrive)
                count = 4 >> stage
                kept = bit_of(HALVED[plan][stage]) * count
                if stage < 2:
                    summed(mine[stage], kept, came[stage], 0, count, mine[stage + 1])
                    each(piece, stage + 1, start)
                else:
                    grads[piece][...] = summed(mine[2], kept, came[2], 0, 1, None)
                continue
            if plan == YD and stage == 1:
                total = mine[1][z].astype(F32)
                each(piece, 1, arrive)
                for k in range(3):
                    total = total + came[1][k].astype(F32)
                grads[piece][...] = total
                continue
            if plan != NY and stage == 0:
                each(piece, 0, arrive)
                summed(mine[0], 4 * y, came[0], 0, 4, mine[1])
                each(piece, 1, start)
                continue
            if plan == NY and stage == 3:
                each(piece, 3, arrive)
                grads[piece][...] = summed(mine[2], y, came[3], 0, 1, None)
                continue
            size = 2 if plan == NY else 1
            step = stage if plan == NY else stage - 1
            pair = mine[1 if plan == NY else 2]
            if step == 0:
                each(piece, stage, arrive)
                summed(mine[0 if plan == NY else 1], 2 * size * facing, came[stage], 0, 2 * size, pair)
                each(piece, stage + 1, start, 1)
                each(piece, stage + 2, start, 0)
            elif step == 1:
                each(piece, stage, arrive, 1)
                each(piece, stage + 1, start, 1)
            else:
                arrive(dp_copies(piece, stage)[0][1]())
                place = (z % 2) * size
                for flag, source in ((1, came[stage - 1]), (0, pair)):

                    @pl.when(inner == flag)
                    def _():
                        if plan == NY:
                            summed(source, place, came[stage], 0, 2, mine[2])
                        else:
                            grads[piece][...] = summed(source, place, came[stage], 0, 1, None)

                if plan == NY:
                    each(piece, stage + 1, start)

    done = [(r.layer_out_v, r.layer_out), (r.feats_grad_v, r.feats_grad), (r.small_out_v, r.small_out)]
    done += list(zip(grads, grad_outs))

    def write_out(i):
        return pltpu.make_async_copy(*done[i], r.out_sem.at[i])

    def poll(point):
        for piece, stage in POLLS[point] if dp_bits else ():
            dp_finish(stage, piece)
            if stage == len(ARRIVING[PLANS[piece]]) - 1:
                write_out(3 + piece).start()

    pl.semaphore_wait(barrier, len(partners))
    load("ow").wait()
    ow_copy(1).start()
    ow_copy(0).start()
    for name in first:
        if name != "ow":
            load(name).wait()
    count = r.counts[0]
    gain_one, shift_one = row_of(r.gain_one), row_of(r.shift_one)
    q_bias = jnp.broadcast_to(row_of(r.q_bias), (128, cols)).T[:, :1]
    v_bias = jnp.broadcast_to(row_of(r.v_bias), (128, cols)).T[:, :1]
    lane = lax.broadcasted_iota(jnp.int32, (HD, BLOCK), 1)
    first_row = lax.broadcasted_iota(jnp.int32, (HD, BLOCK), 0) == 0
    one = jnp.where(first_row, 1.0, 0.0).astype(BF16)

    @pl.loop(0, blocks)
    def _(i):
        here = rows_at(i * BLOCK, BLOCK)
        load_feats(i).wait()
        std_rows, _ = standardized(r.feats[here, :].astype(F32))
        r.std_one[here, :] = std_rows.astype(BF16)
        normed = (std_rows * gain_one + shift_one).astype(BF16)
        r.normed[here, :] = normed
        projected = dot_nt(r.wqkv[...].reshape(3 * cols, width), normed)
        bias = jnp.where(jnp.logical_and(first_row, lane + i * BLOCK >= count), NEG, 0.0).astype(BF16)
        for h in range(heads):
            part = slice(h * HD, (h + 1) * HD)
            of_head = projected[3 * h * HD : 3 * (h + 1) * HD]
            query = ((of_head[:HD] + q_bias[part]).astype(BF16).astype(F32) * SCORE_SCALE).astype(BF16)
            keys = of_head[HD : 2 * HD].astype(BF16)
            values = (of_head[2 * HD :] + v_bias[part]).astype(BF16)
            r.query_t[i, h] = jnp.concatenate([query, one], axis=0)
            r.keys[h, here, :] = jnp.concatenate([keys, bias], axis=0).T
            r.values[h, here, :] = values.T
            r.keys_t[h, :, here] = keys
            r.values_t[h, :, here] = values

    @pl.loop(0, 2)
    def _(turn):
        units = [(block_of(2 * turn + place), h) for place in range(2) for h in range(heads)]
        scores = [dot(r.keys[h], r.query_t[block, h]) for block, h in units]
        for (block, h), score in zip(units, scores):
            peak = jnp.max(score, axis=0, keepdims=True)
            exped = jnp.exp(score - peak)
            total = jnp.sum(exped, axis=0, keepdims=True)
            exped = exped.astype(BF16)
            inverse = 1.0 / total
            r.exped[block, h] = exped
            r.inverse_total[block, h] = inverse
            mixed = dot(r.values_t[h], exped) * inverse
            r.mixed_t[block, pl.ds(pl.multiple_of(m * cols + h * HD, HD), HD), :] = mixed.astype(BF16)
        for place in range(2):
            mx_copy(1, turn, place).start()
            mx_copy(0, turn, place).start()

    for name in second:
        load(name).wait()
    slot = lax.broadcasted_iota(jnp.int32, (BLOCK, width), 0)
    r.key_acc[...] = jnp.zeros_like(r.key_acc)
    r.value_acc[...] = jnp.zeros_like(r.value_acc)

    @pl.loop(0, blocks)
    def _(i):
        here = rows_at(i * BLOCK, BLOCK)
        grad = r.og[here, :]
        grad = jnp.where(slot + i * BLOCK < count, grad.astype(F32), 0.0).astype(BF16)
        r.og[here, :] = grad
        r.hidden_grad[here, :] = dot_nt(grad, r.down[...])

    def mx_forward(turn):
        for place in range(2):
            mx_copy(1, turn, place).wait_recv()
            mx_copy(2, turn, place).start()

    def mx_arrive(kind, turn):
        for place in range(2):
            mx_copy(kind, turn, place).wait_recv()

    ow_copy(1).wait_recv()
    ow_copy(2).start()
    mx_forward(0)
    mx_arrive(0, 1)
    ow_copy(0).wait_recv()
    ow_copy(2).wait_recv()
    mx_arrive(2, 0)

    o_bias = row_of(r.o_bias)
    gain_two, shift_two = row_of(r.gain_two), row_of(r.shift_two)
    up_bias, down_bias = row_of(r.up_bias), row_of(r.down_bias)

    def feed_forward(pair, between):
        places = [rows_at(block_of(k) * BLOCK, BLOCK) for k in pair]
        attended = [dot_tn(r.mixed_t[block_of(k)], r.ow[...]) for k in pair]
        between()
        normed_two = []
        for k, here, value in zip(pair, places, attended):
            resid = r.feats[here, :].astype(F32) + (value + o_bias)
            std_rows, inverse = standardized(resid)
            if k == 0:
                r.resid[...] = resid
                r.std_two[...] = std_rows
                r.inverse_two[...] = inverse
            normed_two.append((std_rows * gain_two + shift_two).astype(BF16))
            r.normed_two[here, :] = normed_two[-1]
        pre_up = [dot(value, r.up[...]) + up_bias for value in normed_two]
        pre_grads = []
        for here, value in zip(places, pre_up):
            hidden, slope = gelu_pair(value)
            r.hidden[here, :] = hidden.astype(BF16)
            pre_grads.append((r.hidden_grad[here, :] * slope).astype(BF16))
            r.pre_grad[here, :] = pre_grads[-1]
        return pre_grads

    def feed_forward_out(k):
        return dot(r.hidden[rows_at(block_of(k) * BLOCK, BLOCK), :], r.down[...])

    pre_grads = feed_forward((3, 2), lambda: None)
    r.bk_tx[0] = dot_nt(pre_grads[0], r.up[...]).astype(BF16)
    rs_copy(BK, 0).start()
    mx_forward(1)
    r.back[...] = dot_nt(pre_grads[1], r.up[...])

    def send_back():
        rs_copy(BK, 0).wait_recv()
        r.bk_tx[1] = (r.back[...] + r.bk_rx[0].astype(F32)).astype(BF16)
        rs_copy(BK, 1).start()

    mx_arrive(0, 0)
    mx_arrive(2, 1)
    pre_grads = feed_forward((1, 0), send_back)

    def grad_tiles(left, right, pieces):
        right_all = right[...]

        @pl.loop(0, 2)
        def _(t):
            value = dot_tn(left[:, rows_at(t * 384, 384)], right_all)
            store_piece(pieces[0], t, value[:, :384])
            store_piece(pieces[1], t, value[:, 384:])

        dp_start(*pieces)

    grad_tiles(r.og, r.hidden, (DOWN0, DOWN1))
    grad_tiles(r.normed_two, r.pre_grad, (UP0, UP1))

    r.ml_tx[0] = feed_forward_out(3).astype(BF16)
    rs_copy(ML, 0).start()
    ml_x = feed_forward_out(2)
    r.bk_tx[2] = dot_nt(r.pre_grad[rows_at(block_of(1) * BLOCK, BLOCK), :], r.up[...]).astype(BF16)
    rs_copy(BK, 2).start()
    rs_copy(ML, 0).wait_recv()
    r.ml_tx[1] = (ml_x + r.ml_rx[0].astype(F32)).astype(BF16)
    r.back[...] = dot_nt(r.pre_grad[own, :], r.up[...])
    r.ml_tx[2] = feed_forward_out(1).astype(BF16)
    rs_copy(ML, 2).start()
    r.ml_own[...] = feed_forward_out(0)
    ones = jnp.ones((8, rows), BF16)
    r.small[6:7, :] = dot(ones, r.pre_grad[...])[:1]

    rs_copy(BK, 2).wait_recv()
    rs_copy(BK, 1).wait_recv()
    back = r.back[...] + r.bk_rx[2].astype(F32) + r.bk_rx[1].astype(F32)
    std_rows, inverse = r.std_two[...], r.inverse_two[...]
    own_grad = r.og[own, :].astype(F32)
    resid_grad = own_grad + norm_back(std_rows, inverse, gain_two, back)
    resid_low = resid_grad.astype(BF16)
    for k in (2, 3, 1):
        target_heads = r.ow[pl.ds(pl.multiple_of(mp_peers[k] * cols, 64), cols), :]
        r.mg_tx[k - 1] = dot_nt(target_heads, resid_low).astype(BF16)
        mg_copy(k).start()
    r.mixed_grad_t[m] = dot_nt(r.ow[own_heads, :], resid_low).astype(BF16)
    r.resid_grad[...] = resid_grad
    r.resid_low[c] = resid_low
    rl_copy().start()
    r.back[...] = back

    def attend_back(block):
        for h in range(heads):
            part = slice(h * HD, (h + 1) * HD)
            exped = r.exped[block, h]
            scaled = (r.mixed_grad_t[block, part, :].astype(F32) * r.inverse_total[block, h]).astype(BF16)
            mixed = r.mixed_t[block, pl.ds(pl.multiple_of(m * cols + h * HD, HD), HD), :]
            inner_product = column_sum(scaled.astype(F32) * mixed.astype(F32))
            prob_grad = dot(r.values[h], scaled)
            score_grad = (exped.astype(F32) * (prob_grad - inner_product)).astype(BF16)
            r.value_acc[h] += dot_nt(scaled, exped)
            r.key_acc[h] += dot_nt(r.query_t[block, h][:HD], score_grad)
            query_grad = dot(r.keys_t[h], score_grad) * SCORE_SCALE
            r.dqkv_t[3 * h * HD : (3 * h + 1) * HD, rows_at(block * BLOCK, BLOCK)] = query_grad.astype(BF16)

    def out_partial(head_rows):
        value = dot(r.mixed_t[m, head_rows, :], r.resid_low[c])
        return value + dot(r.mixed_t[cp, head_rows, :], r.resid_low[1 - c])

    @pl.loop(0, blocks)
    def _(i):
        @pl.when(i == 1)
        def _():
            poll(0)
            mg_copy(1).wait_recv()
            rl_copy().wait_recv()
            r.go_tx[...] = out_partial(pl.ds(pl.multiple_of(xp * cols, 64), cols)).astype(BF16)
            go_copy().start()
            rs_copy(ML, 1).start()

        @pl.when(i == 2)
        def _():
            poll(1)
            mg_copy(2).wait_recv()

        @pl.when(i == 3)
        def _():
            poll(2)
            mg_copy(3).wait_recv()

        attend_back(block_of(i))

    poll(3)

    for h in range(heads):
        row = 3 * h * HD
        r.dqkv_t[row + HD : row + 2 * HD, :] = r.key_acc[h].astype(BF16)
        r.dqkv_t[row + 2 * HD : row + 3 * HD, :] = r.value_acc[h].astype(BF16)
    value = dot(r.dqkv_t[...], r.normed[...])
    if dp_bits:
        value = value.astype(BF16)
    for t in range(2):
        for h in range(heads):
            store_piece(HEAD0 + h, t, value[h * cols : (h + 1) * cols, t * 384 : (t + 1) * 384].T)
    dp_start(HEAD0, HEAD1, HEAD2)
    poll(4)

    for step in range(3):
        rs_copy(BK, step).wait_send()
    r.gain_sum[...] = jnp.zeros_like(r.gain_sum)
    r.shift_sum[...] = jnp.zeros_like(r.shift_sum)

    def input_block(i):
        here = rows_at(block_of(3 - i) * BLOCK, BLOCK)
        part = dot_tn(r.dqkv_t[:, here], r.wqkv[...].reshape(3 * cols, width))

        @pl.when(i == 0)
        def _():
            r.bk_tx[0] = part.astype(BF16)
            rs_copy(IN, 0).start()

        @pl.when(i == 1)
        def _():
            rs_copy(IN, 0).wait_recv()
            r.bk_tx[1] = (part + r.in_rx[0].astype(F32)).astype(BF16)
            rs_copy(IN, 1).start()

        @pl.when(i == 2)
        def _():
            r.bk_tx[2] = part.astype(BF16)
            rs_copy(IN, 2).start()

        @pl.when(i == 3)
        def _():
            r.back[...] = part

        r.gain_sum[...] += column_sum(part * r.std_one[here, :].astype(F32))
        r.shift_sum[...] += column_sum(part)

    input_block(0)
    partial = out_partial(own_heads)
    input_block(1)
    poll(5)

    go_copy().wait_recv()
    value = partial + r.go_rx[...].astype(F32)
    for t in range(2):
        store_piece(OUT, t, value[:, t * 384 : (t + 1) * 384].T)
    dp_start(OUT)
    poll(6)

    r.small[2:3, :] = column_sum(r.resid_low[c].astype(F32))
    r.small[3:4, :] = column_sum(r.back[...] * r.std_two[...])
    r.small[4:5, :] = column_sum(r.back[...])
    r.small[5:6, :] = column_sum(r.og[own, :].astype(F32))

    @pl.loop(0, 2)
    def _(i):
        input_block(i + 2)

    poll(7)

    r.small[0:1, :] = r.gain_sum[...]
    r.small[1:2, :] = r.shift_sum[...]
    bias_sums = dot_nt(jnp.ones((8, rows), BF16), r.dqkv_t[...])[:1]
    q_sums = jnp.concatenate([bias_sums[:, 3 * h * HD : (3 * h + 1) * HD] for h in range(heads)], axis=1)
    v_sums = jnp.concatenate([bias_sums[:, (3 * h + 2) * HD : 3 * (h + 1) * HD] for h in range(heads)], axis=1)
    if dp_bits:
        dp_size = 1 << dp_bits
        share, head_share = width // dp_size, cols // dp_size
        blank = jnp.zeros((1, 128 - 2 * head_share), F32)
        for peer in range(dp_size):
            r.small_tx[peer, 0:7, :share] = r.small[0:7, peer * share : (peer + 1) * share]
            of_peer = slice(peer * head_share, (peer + 1) * head_share)
            r.small_tx[peer, 7:8, :] = jnp.concatenate([q_sums[:, of_peer], v_sums[:, of_peer], blank], axis=1)
        for k in range(1, dp_size):
            sd_copy(k).start()
    else:
        r.small[7:8, :] = jnp.concatenate([q_sums, v_sums, jnp.zeros((1, width - 2 * cols), F32)], axis=1)

    poll(8)
    rs_copy(ML, 1).wait_recv()
    rs_copy(ML, 2).wait_recv()
    mlp = r.ml_own[...] + r.ml_rx[2].astype(F32) + r.ml_rx[1].astype(F32)
    r.layer_out_v[...] = (r.resid[...] + (mlp + down_bias)).astype(BF16)
    write_out(0).start()
    std_rows, inverse = standardized(r.feats[own, :].astype(F32))
    poll(9)

    if dp_bits:
        total = r.small_tx[lax.axis_index(DP)]
        for k in range(1, 1 << dp_bits):
            sd_copy(k).wait_recv()
            total = total + r.sd_rx[k - 1]
        r.small_dp[...] = total
    else:
        r.small_dp[...] = r.small[...]
    for k in mp_peers:
        sg_copy(k).start()

    poll(10)
    rs_copy(IN, 2).wait_recv()
    rs_copy(IN, 1).wait_recv()
    back = r.back[...] + r.in_rx[2].astype(F32) + r.in_rx[1].astype(F32)
    r.feats_grad_v[...] = (r.resid_grad[...] + norm_back(std_rows, inverse, gain_one, back)).astype(BF16)
    write_out(1).start()

    total = r.small_dp[...]
    for k in mp_peers:
        sg_copy(k).wait_recv()
        of_peer = r.sg_rx[k - 1]
        total = total + jnp.where(lax.broadcasted_iota(jnp.int32, of_peer.shape, 0) < 6, of_peer, 0.0)
    r.small_out_v[...] = total
    write_out(2).start()
    poll(11)
    if not dp_bits:
        for piece in range(len(PLANS)):
            write_out(3 + piece).start()

    for i in range(len(done)):
        write_out(i).wait()
    for kind in range(3):
        ow_copy(kind).wait_send()
        rs_copy(IN, kind).wait_send()
        rs_copy(ML, kind).wait_send()
        for turn in range(2):
            for place in range(2):
                mx_copy(kind, turn, place).wait_send()
    rl_copy().wait_send()
    go_copy().wait_send()
    for k in mp_peers:
        mg_copy(k).wait_send()
        sg_copy(k).wait_send()
    if dp_bits:
        for k in range(1, 1 << dp_bits):
            sd_copy(k).wait_send()
        for piece, plan in enumerate(PLANS):
            for stage in range(len(ARRIVING[plan])):
                each(piece, stage, leave)


def finish_kernel(names, *refs):
    r = types.SimpleNamespace(**dict(zip(names, refs)))
    grads = refs[len(names) :]
    shard = r.up.shape[0]
    unpacked = (r.head0, r.head1, r.head2, r.o)
    incoming = [
        (r.small_out, r.small), (r.layer_out, r.layer), (r.feats_grad, r.feats), *zip(grads[HEAD0:], unpacked),
        (grads[UP0], r.up.at[:, pl.ds(0, 384)]), (grads[UP1], r.up.at[:, pl.ds(384, 384)]),
        (grads[DOWN0], r.down.at[:, pl.ds(0, 384)]), (grads[DOWN1], r.down.at[:, pl.ds(384, 384)]),
    ]
    outgoing = [
        (r.layer, r.out_layer), (r.feats, r.out_feats), (r.up, r.out_up), (r.down, r.out_down), (r.q, r.out_q),
        (r.k, r.out_k), (r.v, r.out_v), (r.o_t, r.out_o), (r.up_bias, r.out_up_bias),
    ]
    vectors = (r.out_gain_one, r.out_shift_one, r.out_o_bias, r.out_gain_two, r.out_shift_two, r.out_down_bias, r.out_q_bias,
               r.out_v_bias)
    outgoing += [(r.pieces.at[i], target) for i, target in enumerate(vectors)]

    def take(i):
        return pltpu.make_async_copy(*incoming[i], r.in_sem.at[i])

    def give(i):
        return pltpu.make_async_copy(*outgoing[i], r.out_sem.at[i])

    for i in range(len(incoming)):
        take(i).start()
    take(0).wait()
    m = lax.axis_index(MP)
    small = r.small[...]
    piece = r.out_gain_one.shape[0]
    mine = pltpu.roll(small, (128 - m * piece) % 128, 1)
    for i in range(6):
        r.pieces[i] = mine[i, :piece]
    r.pieces[6] = small[7, :piece]
    r.pieces[7] = small[7, piece : 2 * piece]
    r.up_bias[...] = small[6, :shard]
    for i in range(8, len(outgoing)):
        give(i).start()
    for i in (1, 2):
        take(i).wait()
        give(i - 1).start()
    for i in range(3, 7):
        take(i).wait()
    heads = [jnp.concatenate([ref[:, :192], ref[:, 192:]], axis=0) for ref in unpacked]
    for i, target in enumerate((r.q, r.k, r.v)):
        target[...] = jnp.concatenate([value[:, i * HD : (i + 1) * HD] for value in heads[:3]], axis=1)
        give(4 + i).start()
    r.o_t[...] = heads[3].T
    give(7).start()
    for i in range(7, 11):
        take(i).wait()
        if i % 2 == 0:
            give((i - 4) // 2).start()
    for i in range(len(outgoing)):
        give(i).wait()


def layer_call(dp_size, clip_feats, counts, gain_one, shift_one, q_weight, k_weight, v_weight, q_bias, v_bias, o_weight,
               o_bias, gain_two, shift_two, up_weight, up_bias, down_weight, down_bias, out_grad):
    rows, width = clip_feats.shape
    cols = q_weight.shape[1]
    heads = cols // HD
    hidden_cols = up_weight.shape[1]
    dp_bits = 3 if dp_size == 8 else 0
    vmem = pl.BlockSpec(memory_space=pltpu.VMEM)
    anywhere = pl.BlockSpec(memory_space=pl.ANY)
    by_head = (heads, HD, width)
    inputs = dict(
        gain_one_hbm=(gain_one, anywhere), shift_one_hbm=(shift_one, anywhere), q_bias_hbm=(q_bias, anywhere),
        v_bias_hbm=(v_bias, anywhere), o_bias_hbm=(o_bias, anywhere), gain_two_hbm=(gain_two, anywhere),
        shift_two_hbm=(shift_two, anywhere), up_bias_hbm=(up_bias, anywhere),
        down_bias_hbm=(down_bias, anywhere), counts_hbm=(counts, anywhere),
        feats_hbm=(clip_feats, anywhere), qw_hbm=(q_weight.T.reshape(by_head), anywhere),
        kw_hbm=(k_weight.T.reshape(by_head), anywhere), vw_hbm=(v_weight.T.reshape(by_head), anywhere),
        ow_hbm=(o_weight, anywhere), up_hbm=(up_weight, anywhere),
        down_hbm=(down_weight, anywhere), og_hbm=(out_grad, anywhere),
    )
    shard = width // dp_size if dp_bits else width
    small_shape = (8, 128) if dp_bits else (8, width)
    outputs = dict(layer_out=((BLOCK, width), BF16), feats_grad=((BLOCK, width), BF16), small_out=(small_shape, F32))
    grads = [(packed_shape(i, shard) if dp_bits else (width, COLUMNS[i]), F32) for i in range(len(PLANS))]
    piece = (BLOCK, width)
    scratch = dict(
        gain_one=((width,), BF16), shift_one=((width,), BF16), q_bias=((cols,), BF16), v_bias=((cols,), BF16),
        o_bias=((width,), BF16), gain_two=((width,), BF16), shift_two=((width,), BF16),
        up_bias=((hidden_cols,), BF16), down_bias=((width,), BF16),
        feats=((rows, width), BF16), wqkv=((heads, 3 * HD, width), BF16), ow=((width, width), BF16),
        og=((rows, width), BF16), down=((hidden_cols, width), BF16), up=((width, hidden_cols), BF16),
        normed=((rows, width), BF16), std_one=((rows, width), BF16),
        query_t=((rows // BLOCK, heads, 2 * HD, BLOCK), BF16), keys=((heads, rows, 2 * HD), BF16), values=((heads, rows, HD), BF16),
        keys_t=((heads, HD, rows), BF16), values_t=((heads, HD, rows), BF16), mixed_t=((rows // BLOCK, width, BLOCK), BF16),
        exped=((rows // BLOCK, heads, rows, BLOCK), BF16), inverse_total=((rows // BLOCK, heads, 1, BLOCK), F32), hidden_grad=((rows, hidden_cols), F32), resid=(piece, F32),
        normed_two=((rows, width), BF16), hidden=((rows, hidden_cols), BF16), pre_grad=((rows, hidden_cols), BF16),
        back=(piece, F32), resid_grad=(piece, F32),
        resid_low=((2,) + piece, BF16), go_tx=((cols, width), BF16), go_rx=((cols, width), BF16), std_two=(piece, F32), inverse_two=((BLOCK, 1), F32), ml_own=(piece, F32),
        bk_tx=((3,) + piece, BF16), bk_rx=((3,) + piece, BF16), ml_tx=((3,) + piece, BF16),
        ml_rx=((3,) + piece, BF16), in_rx=((3,) + piece, BF16),
        mg_tx=((3, cols, BLOCK), BF16), mixed_grad_t=((rows // BLOCK, cols, BLOCK), BF16),
        key_acc=((heads, HD, rows), F32), value_acc=((heads, HD, rows), F32), dqkv_t=((3 * cols, rows), BF16),
        gain_sum=((1, width), F32), shift_sum=((1, width), F32),
        small=((8, width), F32), small_dp=(small_shape, F32), sg_rx=((3,) + small_shape, F32),
    )
    scratch.update({name + "_v": spec for name, spec in outputs.items()})
    of_pieces = list(grads)
    if dp_bits:
        scratch.update(
            small_tx=((dp_size,) + small_shape, F32), sd_rx=((dp_size - 1,) + small_shape, F32)
        )
        for table in (HELD, ARRIVING):
            for i, plan in enumerate(PLANS):
                of_pieces += [((count,) + packed_shape(i, shard), BF16) for count in table[plan]]
    copies = 29 + 12 + 4 * len(PLANS)
    scalars = dict(
        counts=pltpu.SMEM((1,), jnp.int32), load_sem=pltpu.SemaphoreType.DMA((17 + rows // BLOCK,)),
        out_sem=pltpu.SemaphoreType.DMA((len(outputs) + len(grads),)), send_sem=pltpu.SemaphoreType.DMA((copies,)),
        recv_sem=pltpu.SemaphoreType.DMA((copies,)),
    )
    names = list(inputs) + list(outputs)
    kernel_names = [*inputs, *outputs, *scratch, *scalars]

    def kernel(*refs):
        refs = list(refs)
        grad_refs = refs[len(names) : len(names) + len(grads)]
        rest = refs[len(names) + len(grads) :]
        named = len(scratch) + len(scalars)
        layer_kernel(kernel_names, dp_bits, *refs[: len(names)], *rest[:named], *grad_refs, *rest[named:])

    results = pl.pallas_call(
        kernel,
        out_shape=[jax.ShapeDtypeStruct(*spec) for spec in [*outputs.values(), *grads]],
        in_specs=[spec for _, spec in inputs.values()],
        out_specs=[anywhere] * (len(outputs) + len(grads)),
        scratch_shapes=[pltpu.VMEM(*spec) for spec in scratch.values()] + list(scalars.values())
        + [pltpu.VMEM(*spec) for spec in of_pieces],
        compiler_params=pltpu.CompilerParams(collective_id=0, has_side_effects=True, vmem_limit_bytes=67043328),
        name="layer",
    )(*[value for value, _ in inputs.values()])
    return dict(zip(outputs, results)), results[len(outputs) :]


def finish_call(out, grads, cols, hidden_cols):
    shard, width = COLUMNS[UP0] // 4, out["layer_out"].shape[1]
    rows = ((BLOCK, width), BF16)
    small = ((shard // 4,), F32)
    head = ((shard, cols), F32)
    shapes = dict(
        out_layer=rows, out_feats=rows, out_gain_one=small, out_shift_one=small, out_q=head, out_k=head, out_v=head,
        out_q_bias=small, out_v_bias=small, out_o=((cols, shard), F32), out_o_bias=small, out_gain_two=small,
        out_shift_two=small, out_up=((shard, hidden_cols), F32), out_up_bias=((shard,), F32),
        out_down=((shard, hidden_cols), F32), out_down_bias=small,
    )
    packed = (packed_shape(OUT, shard), F32)
    scratch = dict(
        small=((8, 128), F32), layer=rows, feats=rows, head0=packed, head1=packed, head2=packed, o=packed,
        up=((shard, hidden_cols), F32), down=((shard, hidden_cols), F32), q=head, k=head, v=head, o_t=((cols, shard), F32),
        up_bias=((shard,), F32), pieces=((8, shard // 4), F32),
    )
    sems = dict(in_sem=pltpu.SemaphoreType.DMA((11,)), out_sem=pltpu.SemaphoreType.DMA((17,)))
    names = [*out, *shapes, *scratch, *sems]

    def kernel(*refs):
        count = len(out) + len(grads)
        finish_kernel(names, *refs[: len(out)], *refs[count:], *refs[len(out) : count])

    anywhere = pl.BlockSpec(memory_space=pl.ANY)
    results = pl.pallas_call(
        kernel,
        out_shape=[jax.ShapeDtypeStruct(*spec) for spec in shapes.values()],
        in_specs=[anywhere] * (len(out) + len(grads)),
        out_specs=[anywhere] * len(shapes),
        scratch_shapes=[pltpu.VMEM(*spec) for spec in scratch.values()] + list(sems.values()),
        name="finish",
    )(*out.values(), *grads)
    return (*results[:15], results[15].T, results[16])


def shards(dp_size, *args):
    out, grads = layer_call(dp_size, *args)
    cols, hidden_cols = args[4].shape[1], args[13].shape[1]
    if dp_size == 8:
        return finish_call(out, grads, cols, hidden_cols)

    def over(value, dim):
        return lax.psum_scatter(value, DP, scatter_dimension=dim, tiled=True)

    small = lax.psum(out["small_out"], DP)
    width = small.shape[1]
    d, m = lax.axis_index(DP), lax.axis_index(MP)
    piece = width // (dp_size * 4)
    group = [lax.dynamic_slice(small, (i, (d * 4 + m) * piece), (1, piece)).reshape(piece) for i in range(6)]
    up_piece = hidden_cols // dp_size
    head_piece = cols // dp_size
    up_bias = lax.dynamic_slice(small, (6, d * up_piece), (1, up_piece)).reshape(up_piece)
    q_bias = lax.dynamic_slice(small, (7, d * head_piece), (1, head_piece)).reshape(head_piece)
    v_bias = lax.dynamic_slice(small, (7, cols + d * head_piece), (1, head_piece)).reshape(head_piece)
    heads = grads[HEAD0 : HEAD2 + 1]
    q_grad, k_grad, v_grad = (
        jnp.concatenate([value[:, i * HD : (i + 1) * HD] for value in heads], axis=1) for i in range(3)
    )
    up_grad = jnp.concatenate([grads[UP0], grads[UP1]], axis=1)
    down_grad = jnp.concatenate([grads[DOWN0], grads[DOWN1]], axis=1)
    return (
        out["layer_out"], out["feats_grad"], group[0], group[1], over(q_grad, 0), over(k_grad, 0), over(v_grad, 0),
        q_bias, v_bias, over(grads[OUT].T, 1), group[2], group[3], group[4], over(up_grad, 0), up_bias,
        over(down_grad.T, 1), group[5],
    )


def solution(mesh):
    placed = (
        P(DP, None), P(DP), P(), P(), P(None, MP), P(None, MP), P(None, MP), P(MP), P(MP), P(MP, None),
        P(), P(), P(), P(None, MP), P(MP), P(MP, None), P(), P(DP, None),
    )
    return jax.shard_map(
        functools.partial(shards, mesh.shape[DP]),
        mesh=mesh,
        in_specs=placed,
        out_specs=(
            P((DP, MP), None), P((DP, MP), None), P((DP, MP)), P((DP, MP)), P(DP, MP), P(DP, MP),
            P(DP, MP), P((MP, DP)), P((MP, DP)), P(MP, DP), P((DP, MP)), P((DP, MP)),
            P((DP, MP)), P(DP, MP), P((MP, DP)), P(MP, DP), P((DP, MP)),
        ),
        check_vma=False,
    )
```
